1024 devices in a mesh: gx: 16 (over x, core), gy: 8 (over z), gz: 8 (over y).
Axes of the slice: x: 8, y: 8, z: 8, core: 2. Of those that a mesh axis runs over, the one named last changes fastest.
Arguments:
- divergence: float32 [256, 128, 1024], P('gx', 'gy', 'gz'), may hold values from -6 to 6
- damping: float32 [256, 128, 1024], P('gx', 'gy', 'gz'), may hold values from 5e-06 to 0.004
Outputs:
- potential: float32 [256, 128, 1024], P('gx', 'gy', 'gz')
The draws below stay inside these ranges and needn't reach their ends.
All inputs are finite; a program needn't handle non-finite values.
Results may differ from the reference program's by a relative error of at most 0.0001.
Values sent between devices are 32-bit elements; how exact they have to be, the bound alone decides.
A program may use at most 64 MiB of HBM per device.

```python
import math
import jax
import jax.numpy as jnp
from jax import lax

CX = 16
CY = 16
CZ = 128
LEVELS = 4
PRE = 2
POST = 2
NX = 256
NY = 128
NZ = 1024


def smooth_field(key, size_x, size_y, size_z):
    keys = jax.random.split(key, 3)
    freqs = jax.random.randint(keys[0], (3, 3), 1, 3).astype(jnp.float32)
    phases = jax.random.uniform(keys[1], (3, 3), jnp.float32, 0.0, 2.0 * math.pi)
    weights = jax.random.uniform(keys[2], (3,), jnp.float32, 0.5, 1.0)
    coord_x = (jnp.arange(size_x, dtype=jnp.float32) + 0.5) / size_x
    coord_y = (jnp.arange(size_y, dtype=jnp.float32) + 0.5) / size_y
    coord_z = (jnp.arange(size_z, dtype=jnp.float32) + 0.5) / size_z
    total = jnp.zeros((size_x, size_y, size_z), jnp.float32)
    for term_index in range(3):
        along_x = jnp.cos(2.0 * math.pi * freqs[term_index, 0] * coord_x + phases[term_index, 0])
        along_y = jnp.cos(2.0 * math.pi * freqs[term_index, 1] * coord_y + phases[term_index, 1])
        along_z = jnp.cos(2.0 * math.pi * freqs[term_index, 2] * coord_z + phases[term_index, 2])
        total = total + weights[term_index] * along_x[:, None, None] * along_y[None, :, None] * along_z[None, None, :]
    return total / jnp.sum(weights)


def draw_divergence(key, part):
    rough_key = jax.random.fold_in(key, 11)
    smooth_key = jax.random.fold_in(key, 12)
    strength = 2.0 * (9.87 * (1.0 / (NX * NX) + 1.0 / (NY * NY) + 1.0 / (NZ * NZ)) + 0.0003)
    smooth = smooth_field(smooth_key, NX, NY, NZ)
    rough = jnp.clip(jax.random.normal(rough_key, (NX, NY, NZ), jnp.float32), -4.0, 4.0)
    broad = strength * 2.0 * smooth
    return rough + broad


def draw_damping(key, part):
    rough_key = jax.random.fold_in(key, 21)
    smooth_key = jax.random.fold_in(key, 22)
    smooth = smooth_field(smooth_key, NX, NY, NZ)
    rough = jnp.tanh(jax.random.normal(rough_key, (NX, NY, NZ), jnp.float32))
    share = 0.5 + 0.299 * rough + 0.2 * smooth
    return jnp.exp(math.log(5e-06) + math.log(800.0) * share)


def setup_inputs(seed: int = 0) -> dict:
    splits = jax.random.split(jax.random.key(seed), 3)
    return {
        "divergence": draw_divergence(jax.random.fold_in(splits[2], 71), 0),
        "damping": draw_damping(jax.random.fold_in(splits[2], 71), 0),
    }


relax_weight = 2.0 / 3.0

def neighbour_sum(padded):
    total = padded[2:, 1:-1, 1:-1] + padded[:-2, 1:-1, 1:-1]
    total = total + padded[1:-1, 2:, 1:-1] + padded[1:-1, :-2, 1:-1]
    total = total + padded[1:-1, 1:-1, 2:] + padded[1:-1, 1:-1, :-2]
    return total

def apply_level(values, padded, damping_level, coupling):
    return (6.0 * values - neighbour_sum(padded)) * coupling + damping_level * values

def relaxed_sweep(values, padded, source, damping_level, coupling):
    diagonal = 6.0 * coupling + damping_level
    return values + relax_weight * (source - apply_level(values, padded, damping_level, coupling)) / diagonal

def coarsen(values, block_x, block_y, block_z):
    size_x, size_y, size_z = values.shape
    shaped = values.reshape(size_x // block_x, block_x, size_y // block_y, block_y, size_z // block_z, block_z)
    return shaped.mean(axis=(1, 3, 5))

def refine(values, block_x, block_y, block_z):
    return jnp.repeat(jnp.repeat(jnp.repeat(values, block_x, 0), block_y, 1), block_z, 2)

def sine_table(points, dtype):
    indices = jnp.arange(points, dtype=dtype) + 1.0
    return math.sqrt(2.0 / (points + 1)) * jnp.sin(math.pi * indices[:, None] * indices[None, :] / (points + 1))

def eigen_values(points, spacing, dtype):
    indices = jnp.arange(points, dtype=dtype) + 1.0
    return (2.0 - 2.0 * jnp.cos(math.pi * indices / (points + 1))) / (spacing * spacing)

def coarse_solve(source, damping_mean, spacing_x, spacing_y, spacing_z):
    size_x, size_y, size_z = source.shape
    dtype = source.dtype
    table_x = sine_table(size_x, dtype)
    table_y = sine_table(size_y, dtype)
    table_z = sine_table(size_z, dtype)
    spectrum = jnp.einsum('ai,bj,ck,ijk->abc', table_x, table_y, table_z, source, precision=lax.Precision.HIGHEST)
    denominator = eigen_values(size_x, spacing_x, dtype)[:, None, None] + eigen_values(size_y, spacing_y, dtype)[None, :, None] + eigen_values(size_z, spacing_z, dtype)[None, None, :] + damping_mean
    spectrum = spectrum / denominator
    return jnp.einsum('ia,jb,kc,abc->ijk', table_x, table_y, table_z, spectrum, precision=lax.Precision.HIGHEST)

def reference(divergence, damping):
    dampings = [damping]
    for level_index in range(1, LEVELS):
        dampings.append(coarsen(dampings[-1], 2, 2, 2))
    sources = []
    smoothed = []
    source = divergence
    for level_index in range(LEVELS):
        coupling = 0.25 ** level_index
        values = relax_weight * source / (6.0 * coupling + dampings[level_index])
        for sweep_index in range(PRE - 1):
            values = relaxed_sweep(values, jnp.pad(values, 1), source, dampings[level_index], coupling)
        remainder = source - apply_level(values, jnp.pad(values, 1), dampings[level_index], coupling)
        sources.append(source)
        smoothed.append(values)
        source = coarsen(remainder, 2, 2, 2)
    shrink = 2 ** (LEVELS - 1)
    block_x, block_y, block_z = (CX // shrink, CY // shrink, CZ // shrink)
    coarse_source = coarsen(remainder, block_x, block_y, block_z)
    damping_mean = jnp.mean(coarsen(dampings[-1], block_x, block_y, block_z))
    solution = coarse_solve(coarse_source, damping_mean, CX, CY, CZ)
    correction = refine(solution, block_x, block_y, block_z)
    for level_index in reversed(range(LEVELS)):
        coupling = 0.25 ** level_index
        values = smoothed[level_index] + correction
        for sweep_index in range(POST):
            values = relaxed_sweep(values, jnp.pad(values, 1), sources[level_index], dampings[level_index], coupling)
        if level_index > 0:
            correction = refine(values, 2, 2, 2)
    return values
```

```python
import functools
import itertools
import math

import jax
import jax.numpy as jnp
import numpy as np
from jax import lax
from jax.experimental import pallas as pl
from jax.experimental.pallas import tpu as pltpu
from jax.sharding import PartitionSpec as P

MESH = pl.DeviceIdType.MESH
HI = lax.Precision.HIGHEST
LEVELS = 4
LANES = 128
RELAX = 2.0 / 3.0
SIZE = (16, 8, 4, 2)
DEPTH = (128, 64, 32, 16)
HALO = (3, 4, 4, 2)
ROW = (4, 4, 4, 2)
PLANES = tuple(n + 2 * r for n, r in zip(SIZE, HALO))
ROWS = (24, 16, 16, 8)
OFFSETS = [o for o in itertools.product((-1, 0, 1), repeat=3) if o != (0, 0, 0)]
FLAT = [o for o in OFFSETS if o[2] == 0]
TALL = [o for o in OFFSETS if o[2] != 0]


def iota(shape, axis):
    return lax.broadcasted_iota(jnp.int32, shape, axis)


def neighbour_sum(v):
    c = v[1:-1]
    rows, lanes = c.shape[1], c.shape[2]
    total = v[2:] + v[:-2]
    total = total + (pltpu.roll(c, 1, 1) + pltpu.roll(c, rows - 1, 1))
    return total + (pltpu.roll(c, 1, 2) + pltpu.roll(c, lanes - 1, 2))


def sweep(v, b, w):
    return v[1:-1] * (1.0 / 3.0) + w * (b + neighbour_sum(v))


def pair_planes(v):
    n = v.shape[0]
    halves = v.reshape(n // 2, 2, v.shape[1], v.shape[2])
    return halves[:, 0] + halves[:, 1]


def lanes_dot(v, table):
    planes, rows, lanes = v.shape
    out = jnp.dot(
        v.reshape(planes * rows, lanes), table, precision=HI, preferred_element_type=jnp.float32
    )
    return out.reshape(planes, rows, table.shape[1])


def refine_table(lanes, turn):
    fine = iota((LANES, lanes), 1)
    place = jnp.where(fine < turn, fine, fine - lanes)
    coarse = jnp.bitwise_and(place + 2 * LANES, 1)
    coarse = (place + 2 * LANES - coarse) // 2 % LANES
    return (iota((LANES, lanes), 0) == coarse).astype(jnp.float32)


def kernel(counts, b_hbm, d_hbm, tab_ref, out_ref, *refs):
    NX, NY, NZ = counts
    NXP = max(8, NX)
    it = iter(refs)
    eb, ed, e1, e2, e3, u2, u3, x3 = (next(it) for _ in range(8))
    zs = [next(it) for _ in range(7)]
    zr = [next(it) for _ in range(7)]
    bx = [next(it) for _ in range(4)]
    wx = [next(it) for _ in range(4)]
    vx = [next(it) for _ in range(4)]
    pair, fine0 = next(it), next(it)
    row0, row1, row2, g1, g2, g3 = (next(it) for _ in range(6))
    tally = next(it)
    send_sem, recv_sem, line_send, line_recv, in_sem = (next(it) for _ in range(5))

    gx, gy, gz = lax.axis_index("gx"), lax.axis_index("gy"), lax.axis_index("gz")

    places = {}
    for name, here, count in zip(("gx", "gy", "gz"), (gx, gy, gz), counts):
        places[name, 0] = here
        for step in range(1, count):
            moved = here + step
            places[name, step] = jnp.where(moved >= count, moved - count, moved)

    def device(offset):
        return tuple(
            places[name, step % count]
            for name, count, step in zip(("gx", "gy", "gz"), counts, offset)
        )

    for ref in (eb, ed, e1, e2, e3, u2, u3, x3, pair, *zs, *zr):
        ref[...] = jnp.zeros(ref.shape, jnp.float32)
    n = SIZE[0]
    loads = []
    for k, (src, dst) in enumerate(((b_hbm, eb), (d_hbm, ed))):
        load = pltpu.make_async_copy(
            src, dst.at[pl.ds(HALO[0], n), pl.ds(ROW[0], n)], in_sem.at[k]
        )
        load.start()
        loads.append(load)

    peers = set()
    for o in OFFSETS:
        peers.add(tuple(s % c for s, c in zip(o, counts)))
    for axis in range(3):
        for k in range(1, counts[axis]):
            peers.add(tuple(k if a == axis else 0 for a in range(3)))
    peers.discard((0, 0, 0))
    barrier = pltpu.get_barrier_semaphore()
    for o in sorted(peers):
        pl.semaphore_signal(barrier, inc=1, device_id=device(o), device_id_type=MESH)

    lane = iota((1, LANES), 1)
    low = jnp.bitwise_and(lane, 63)
    halve = (
        iota((LANES, LANES), 0) // 2 == iota((LANES, LANES), 1)
    ).astype(jnp.float32) * 0.5

    def coarsen_own(level, values, first):
        half = SIZE[level] // 2
        rows = values.shape[1]
        pair[0:half, 0:rows, :] = pair_planes(values)
        top = pair[0:half, pl.ds(first, 8, stride=2), :]
        top = top + pair[0:half, pl.ds(first + 1, 8, stride=2), :]
        return lanes_dot(top, halve)

    def pack(level, which, fields):
        r, bz = HALO[level], DEPTH[level]
        joined = len(fields) == 1
        for side in range(2):
            start = bz - r if side else 0
            acc = jnp.zeros((SIZE[level], LANES), jnp.float32)
            for x in range(SIZE[level]):
                for f, values in enumerate(fields):
                    place = f * 64 + x * r
                    shift = (place - start) % LANES
                    moved = values[x] if shift == 0 else pltpu.roll(values[x], shift, 1)
                    seat = low if joined else lane - f * 64
                    acc = jnp.where((seat >= x * r) & (seat < x * r + r), moved, acc)
            zs[which][side, :, :] = acc

    def unpack(level, which, f):
        n, r, bz = SIZE[level], HALO[level], DEPTH[level] % LANES
        planes = []
        for p in range(PLANES[level]):
            block, x = divmod(p - r + n, n)
            seat = f * 64 + x * r
            down = (LANES - r - seat) % LANES
            up = (bz - seat) % LANES
            below, above = zr[which][0, block], zr[which][1, block]
            below = pltpu.roll(below, down, 1) if down else below
            above = pltpu.roll(above, up, 1) if up else above
            inner = jnp.where((lane >= bz) & (lane < bz + r), above, 0.0)
            planes.append(jnp.where(lane >= LANES - r, below, inner))
        return jnp.stack(planes, axis=0)

    def span(step, n, r):
        return ((0, n), (n - r, r), (0, r))[step]

    unsent = {}

    def drain(sem, rows):
        pltpu.make_async_copy(tally.at[pl.ds(0, rows)], tally.at[pl.ds(0, rows)], sem).wait()

    def sent(turn_set):
        if turn_set in unsent:
            drain(send_sem.at[turn_set], unsent.pop(turn_set))

    def exchange(level, which, blocks, turn_set):
        n, r, row = SIZE[level], HALO[level], ROW[level]
        sent(turn_set)
        sems = dict(send_sem=send_sem.at[turn_set], recv_sem=recv_sem.at[turn_set])
        copies, rows = [], 0
        for o in TALL:
            sy, cy = span(o[1], n, r)
            up = o[2] > 0
            rows += cy
            copies.append(
                pltpu.make_async_remote_copy(
                    src_ref=zs[which].at[1 if up else 0, pl.ds(sy, cy)],
                    dst_ref=zr[which].at[
                        0 if up else 1, 1 - o[0], pl.ds(row + sy - o[1] * n, cy)
                    ],
                    device_id=device(o),
                    device_id_type=MESH,
                    **sems,
                )
            )
        for o in FLAT:
            sx, cx = span(o[0], n, r)
            sy, cy = span(o[1], n, r)
            for block in blocks:
                rows += cx * cy
                copies.append(
                    pltpu.make_async_remote_copy(
                        src_ref=block.at[pl.ds(r + sx, cx), pl.ds(row + sy, cy)],
                        dst_ref=block.at[
                            pl.ds(r + sx - o[0] * n, cx), pl.ds(row + sy - o[1] * n, cy)
                        ],
                        device_id=device(o),
                        device_id_type=MESH,
                        **sems,
                    )
                )
        for copy in copies:
            copy.start()
        unsent[turn_set] = rows
        return turn_set, rows

    def finish(pending):
        drain(recv_sem.at[pending[0]], pending[1])

    def domain(level):
        n, r, row, bz = SIZE[level], HALO[level], ROW[level], DEPTH[level]
        lanes = 256 if level == 0 else LANES
        px = iota((PLANES[level], 1, 1), 0) - r
        py = iota((1, ROWS[level], 1), 1) - row
        pz = iota((1, 1, lanes), 2)
        pz = jnp.where(pz < bz + 32, pz, pz - lanes)
        ok = None
        for p, here, count, size in ((px, gx, NX, n), (py, gy, NY, n), (pz, gz, NZ, bz)):
            at = p + here * size
            good = (p >= -r) & (p < size + r) & (at >= 0) & (at < count * size)
            ok = good if ok is None else ok & good
        return ok

    def presmooth(level, b, d):
        n, r = SIZE[level], HALO[level]
        diag = 6.0 + d
        w = jnp.where(domain(level), RELAX / diag, 0.0)
        bx[level][...] = b
        wx[level][...] = w
        v = w * b
        v = sweep(v, b[1:-1], w[1:-1])
        vx[level][...] = v
        near = v[r - 2 : r + n]
        own = near[1:-1]
        return (b[r : r + n] - diag[r : r + n] * own + neighbour_sum(near))[:, :, :LANES]

    own_damping = []
    for load in loads:
        load.wait()
    d_own = ed[pl.ds(HALO[0], n), pl.ds(ROW[0], n), :]
    pack(0, 0, (eb[pl.ds(HALO[0], n), pl.ds(ROW[0], n), :], d_own))
    pl.semaphore_wait(barrier, len(peers))
    copies = exchange(0, 0, (eb, ed), 0)

    values = d_own
    for level in range(LEVELS - 1):
        coarse = coarsen_own(level, values, 0)
        own_damping.append(coarse)
        values = coarse
    d_last = own_damping[-1]
    own_nodes = (iota((8, LANES), 0) < SIZE[3]) & (iota((8, LANES), 1) < DEPTH[3])
    last_scale = 0.25 ** (LEVELS - 1) / (SIZE[3] * SIZE[3] * DEPTH[3])

    def block_mean(planes, good):
        total = jnp.where(good, sum(planes[k] for k in range(planes.shape[0])), 0.0)
        total = jnp.sum(jnp.sum(total, axis=0, keepdims=True), axis=1, keepdims=True)
        return total * last_scale

    damping_mean = block_mean(d_last, own_nodes)

    finish(copies)
    b0 = jnp.concatenate([eb[...], unpack(0, 0, 0)], axis=2)
    d0 = jnp.concatenate([ed[...], unpack(0, 0, 1)], axis=2)
    remainder = presmooth(0, b0, d0)

    hidden = None
    for level, block in ((1, e1), (2, e2), (3, e3)):
        n, r, row, bz = SIZE[level], HALO[level], ROW[level], DEPTH[level]
        coarse = coarsen_own(level - 1, remainder, ROW[level - 1])
        both = jnp.where(lane < 64, coarse, pltpu.roll(own_damping[level - 1], 64, 2))
        both = both[:, :n]
        block[pl.ds(r, n), pl.ds(row, n), :] = both
        pack(level, level, (both,))
        copies = exchange(level, level, (block,), (0, 1, 2, 1)[level])
        finish(copies)
        e = block[...]
        b = jnp.where(lane < bz, e, unpack(level, level, 0))
        d = jnp.where(lane < bz, pltpu.roll(e, 64, 2), unpack(level, level, 1))
        remainder = presmooth(level, b, d)
        if level >= 2:
            own = vx[level][pl.ds(r - 1, n), pl.ds(row, n), :]
            which = level + 2
            target = (u2, u3)[level - 2]
            target[pl.ds(r, n), pl.ds(row, n), :] = own
            pack(level, which, (own,))
            if hidden is not None:
                finish(hidden)
            hidden = exchange(level, which, (target,), (0, 2)[level - 2])

    source = block_mean(
        remainder,
        (iota((8, LANES), 0) >= ROW[3])
        & (iota((8, LANES), 0) < ROW[3] + SIZE[3])
        & (iota((8, LANES), 1) < DEPTH[3]),
    )

    def send_line(axis, src, dst):
        here, count = (gx, gy, gz)[axis], counts[axis]
        for k in range(1, count):
            offset = tuple(k if a == axis else 0 for a in range(3))
            pltpu.make_async_remote_copy(
                src_ref=src.at[pl.ds(0, 1)],
                dst_ref=dst.at[pl.ds(here, 1)],
                send_sem=line_send.at[axis],
                recv_sem=line_recv.at[axis],
                device_id=device(offset),
                device_id_type=MESH,
            ).start()

    def finish_line(axis):
        drain(line_recv.at[axis], counts[axis] - 1)

    def line_rows(axis, own, dst):
        here, count = (gx, gy, gz)[axis], counts[axis]
        rows = iota(dst.shape, 0)
        got = jnp.where(rows == here, own, dst[...])
        return jnp.where(rows < count, got, 0.0), rows

    own0 = jnp.where(lane < 64, source, damping_mean)
    row0[...] = jnp.broadcast_to(own0, (8, LANES))
    send_line(2, row0, g1)
    finish_line(2)
    got, rows = line_rows(2, own0, g1)
    own1 = jnp.sum(
        jnp.where((lane >= 64) | (lane % NZ == rows), got, 0.0), axis=0, keepdims=True
    )
    row1[...] = jnp.broadcast_to(own1, (8, LANES))
    send_line(1, row1, g2)
    finish_line(1)
    got, rows = line_rows(1, own1, g2)
    own2 = jnp.sum(
        jnp.where((lane >= 64) | (lane // NZ == rows), got, 0.0), axis=0, keepdims=True
    )
    row2[...] = jnp.broadcast_to(own2, (8, LANES))
    send_line(0, row2, g3)
    finish(hidden)
    finish_line(0)
    got, rows = line_rows(0, own2, g3)
    mean = jnp.sum(got, axis=0, keepdims=True) * (1.0 / (NX * NY * NZ))
    mean = jnp.where(lane < 64, pltpu.roll(mean, 64, 1), 0.0)
    table_x = tab_ref[0:NXP, 0:NXP]
    table_yz = tab_ref[pl.ds(16, LANES), :]
    eigen = tab_ref[pl.ds(16 + LANES, NXP), :]
    dot = functools.partial(jnp.dot, precision=HI, preferred_element_type=jnp.float32)
    spectrum = dot(dot(table_x, jnp.where(lane < NY * NZ, got, 0.0)), table_yz)
    spectrum = spectrum / (eigen + mean)
    coarse = dot(dot(table_x, spectrum), table_yz)

    pick = iota((8, NXP), 1) == gx - 1 + iota((8, NXP), 0) // 2
    along_x = dot(pick.astype(jnp.float32), coarse)
    wanted = iota((8, LANES), 1) // NZ == gy - 1 + iota((8, LANES), 0) // 2
    spread = jnp.stack(
        [
            jnp.where(wanted, jnp.broadcast_to(along_x[p : p + 1], (8, LANES)), 0.0)
            for p in range(PLANES[3])
        ],
        axis=0,
    )
    lane_to = iota((LANES, LANES), 1)
    block_z = jnp.where(lane_to < DEPTH[3], 0, jnp.where(lane_to < 64, 1, -1))
    seat = iota((LANES, LANES), 0) % NZ == gz + block_z
    correction = lanes_dot(spread, seat.astype(jnp.float32))

    def halo_values(level, block, which):
        return jnp.where(lane < DEPTH[level], block[...], unpack(level, which, 0))

    def postsmooth(level, v, start):
        for _ in range(2):
            start = start + 1
            count = v.shape[0] - 2
            v = sweep(v, bx[level][pl.ds(start, count)], wx[level][pl.ds(start, count)])
        return v

    def in_domain(level, v):
        return jnp.where(domain(level), v, 0.0)

    v = in_domain(3, halo_values(3, u3, 5) + correction)
    v = postsmooth(3, v, 0)
    own = v[:, ROW[3] : ROW[3] + SIZE[3]]
    x3[pl.ds(HALO[3], SIZE[3]), pl.ds(ROW[3], SIZE[3]), :] = own
    pack(3, 6, (own,))
    copies = exchange(3, 6, (x3,), 0)
    finish(copies)
    v = in_domain(3, halo_values(3, x3, 6))

    def refined(level, v, first):
        lanes = 256 if level == 0 else LANES
        table = refine_table(lanes, DEPTH[level] + 32)
        planes = v.shape[0]
        wide = lanes_dot(v, table)
        count = ROWS[level] // 2
        parts = []
        for half in range(lanes // LANES):
            piece = wide[:, first : first + count, half * LANES : (half + 1) * LANES]
            fine0[0:planes, pl.ds(0, count, stride=2), :] = piece
            fine0[0:planes, pl.ds(1, count, stride=2), :] = piece
            parts.append(fine0[0:planes, 0 : ROWS[level], :])
        full = parts[0] if len(parts) == 1 else jnp.concatenate(parts, axis=2)
        full = jnp.broadcast_to(full[:, None], (planes, 2, ROWS[level], lanes))
        return full.reshape(2 * planes, ROWS[level], lanes)

    v = halo_values(2, u2, 4) + refined(2, v, 0)
    v = postsmooth(2, in_domain(2, v), 0)
    correction = refined(1, v, ROW[2] - 2)
    v = vx[1][...] + correction[1:-1]
    v = postsmooth(1, v, 1)
    correction = refined(0, v, ROW[1] - 2)
    v = vx[0][...] + correction
    v = postsmooth(0, v, 1)
    for axis in range(3):
        drain(line_send.at[axis], counts[axis] - 1)
    for turn_set in list(unsent):
        sent(turn_set)
    out_ref[...] = v[:, ROW[0] : ROW[0] + SIZE[0], :LANES]


def tables(counts):
    def sine(points):
        index = np.arange(1, points + 1)
        return math.sqrt(2.0 / (points + 1)) * np.sin(
            math.pi * index[:, None] * index[None, :] / (points + 1)
        )

    def eigen(points, spacing):
        index = np.arange(1, points + 1)
        return (2.0 - 2.0 * np.cos(math.pi * index / (points + 1))) / (spacing * spacing)

    nx, ny, nz = counts
    out = np.zeros((16 + LANES + 16, LANES))
    out[:nx, :nx] = sine(nx)
    out[16 : 16 + ny * nz, : ny * nz] = np.kron(sine(ny), sine(nz))
    plane = eigen(ny, 16.0)[:, None] + eigen(nz, 128.0)[None, :]
    out[16 + LANES :] = 1.0
    out[16 + LANES : 16 + LANES + nx, : ny * nz] = eigen(nx, 16.0)[:, None] + plane.reshape(1, -1)
    return out.astype(np.float32)


def solution(mesh):
    counts = tuple(mesh.shape[a] for a in ("gx", "gy", "gz"))
    NXP = max(8, counts[0])
    f32 = jnp.float32

    def local(divergence, damping):
        ext = [(p, r, LANES) for p, r in zip(PLANES, ROWS)]
        levels = (0, 1, 2, 3, 2, 3, 3)
        wide = [(p, r, 256 if k == 0 else LANES) for k, (p, r) in enumerate(zip(PLANES, ROWS))]
        inner = [(p - 2, r, z) for p, r, z in wide]
        shapes = [ext[0], ext[0], ext[1], ext[2], ext[3], ext[2], ext[3], ext[3]]
        shapes += [(2, SIZE[k], LANES) for k in levels]
        shapes += [(2, 3, ROWS[k], LANES) for k in levels]
        shapes += wide + wide + inner
        shapes += [(8, 24, LANES), (12, 24, LANES)]
        shapes += [(8, LANES)] * 3
        shapes += [(8, LANES), (8, LANES), (NXP, LANES), (2048, LANES)]
        dma = pltpu.SemaphoreType.DMA
        sems = [dma((3,)), dma((3,)), dma((3,)), dma((3,)), dma((2,))]
        return pl.pallas_call(
            functools.partial(kernel, counts),
            out_shape=jax.ShapeDtypeStruct(divergence.shape, f32),
            in_specs=[
                pl.BlockSpec(memory_space=pl.ANY),
                pl.BlockSpec(memory_space=pl.ANY),
                pl.BlockSpec(memory_space=pltpu.VMEM),
            ],
            out_specs=pl.BlockSpec(memory_space=pltpu.VMEM),
            scratch_shapes=[pltpu.VMEM(s, f32) for s in shapes] + sems,
            compiler_params=pltpu.CompilerParams(
                collective_id=0, has_side_effects=True, vmem_limit_bytes=48 * 1024 * 1024
            ),
            name="vcycle",
        )(divergence, damping, jnp.asarray(tables(counts)))

    spec = P("gx", "gy", "gz")
    return jax.shard_map(
        local, mesh=mesh, in_specs=(spec, spec), out_specs=spec, check_vma=False
    )
```

```python
import functools
import itertools
import math

import jax
import jax.numpy as jnp
import numpy as np
from jax import lax
from jax.experimental import pallas as pl
from jax.experimental.pallas import tpu as pltpu
from jax.sharding import PartitionSpec as P

MESH = pl.DeviceIdType.MESH
HI = lax.Precision.HIGHEST
LEVELS = 4
LANES = 128
RELAX = 2.0 / 3.0
SIZE = (16, 8, 4, 2)
DEPTH = (128, 64, 32, 16)
HALO = (3, 6, 4, 2)
ROW = (4, 8, 4, 2)
PLANES = tuple(n + 2 * r for n, r in zip(SIZE, HALO))
ROWS = (24, 24, 16, 8)
PITCH = (64, 64, 32, 64)
OFFSETS = [o for o in itertools.product((-1, 0, 1), repeat=3) if o != (0, 0, 0)]
FLAT = [o for o in OFFSETS if o[2] == 0]
TALL = [o for o in OFFSETS if o[2] != 0]


def iota(shape, axis):
    return lax.broadcasted_iota(jnp.int32, shape, axis)


def neighbour_sum(v):
    c = v[1:-1]
    rows, lanes = c.shape[1], c.shape[2]
    total = v[2:] + v[:-2]
    total = total + (pltpu.roll(c, 1, 1) + pltpu.roll(c, rows - 1, 1))
    return total + (pltpu.roll(c, 1, 2) + pltpu.roll(c, lanes - 1, 2))


def sweep(v, b, w):
    return v[1:-1] * (1.0 / 3.0) + w * (b + neighbour_sum(v))


def pair_planes(v):
    n = v.shape[0]
    halves = v.reshape(n // 2, 2, v.shape[1], v.shape[2])
    return halves[:, 0] + halves[:, 1]


def lanes_dot(v, table):
    planes, rows, lanes = v.shape
    out = jnp.dot(
        v.reshape(planes * rows, lanes), table, precision=HI, preferred_element_type=jnp.float32
    )
    return out.reshape(planes, rows, table.shape[1])


def refine_table(lanes, turn):
    fine = iota((LANES, lanes), 1)
    place = jnp.where(fine < turn, fine, fine - lanes)
    coarse = jnp.bitwise_and(place + 2 * LANES, 1)
    coarse = (place + 2 * LANES - coarse) // 2 % LANES
    return (iota((LANES, lanes), 0) == coarse).astype(jnp.float32)


def kernel(counts, b_hbm, d_hbm, tab_hbm, out_ref, *refs):
    NX, NY, NZ = counts
    NXP = max(8, NX)
    it = iter(refs)
    eb, ed, e1, e3, u2, u3, tab_ref = (next(it) for _ in range(7))
    zs = [next(it) for _ in range(4)]
    zr = [next(it) for _ in range(4)]
    bx = [next(it) for _ in range(3)]
    wx = [next(it) for _ in range(3)]
    vx = [next(it) for _ in range(3)]
    pair, fine0 = next(it), next(it)
    row0, row1, row2, g1, g2, g3 = (next(it) for _ in range(6))
    tally = next(it)
    send_sem, recv_sem, line_send, line_recv, in_sem = (next(it) for _ in range(5))

    gx, gy, gz = lax.axis_index("gx"), lax.axis_index("gy"), lax.axis_index("gz")

    places = {}
    for name, here, count in zip(("gx", "gy", "gz"), (gx, gy, gz), counts):
        places[name, 0] = here
        for step in range(1, count):
            moved = here + step
            places[name, step] = jnp.where(moved >= count, moved - count, moved)

    def device(offset):
        return tuple(
            places[name, step % count]
            for name, count, step in zip(("gx", "gy", "gz"), counts, offset)
        )

    for ref in (eb, ed, e1, e3, u2, u3, pair, *zs, *zr):
        ref[...] = jnp.zeros(ref.shape, jnp.float32)
    n = SIZE[0]
    loads = []
    for k, (src, dst) in enumerate(((b_hbm, eb), (d_hbm, ed))):
        load = pltpu.make_async_copy(
            src, dst.at[pl.ds(HALO[0], n), pl.ds(ROW[0], n)], in_sem.at[k]
        )
        load.start()
        loads.append(load)
    table_load = pltpu.make_async_copy(tab_hbm, tab_ref, in_sem.at[2])
    table_load.start()

    peers = set()
    for o in OFFSETS:
        peers.add(tuple(s % c for s, c in zip(o, counts)))
    for axis in range(3):
        for k in range(1, counts[axis]):
            peers.add(tuple(k if a == axis else 0 for a in range(3)))
    peers.discard((0, 0, 0))
    barrier = pltpu.get_barrier_semaphore()
    for o in sorted(peers):
        pl.semaphore_signal(barrier, inc=1, device_id=device(o), device_id_type=MESH)

    lane = iota((1, LANES), 1)
    source_lane = iota((LANES, LANES), 0)
    whole = (source_lane // 2 == iota((LANES, LANES), 1)).astype(jnp.float32) * 0.5
    turned = source_lane // 2 + jnp.where(source_lane < 96, 0, 64)
    turned = (turned == iota((LANES, LANES), 1)).astype(jnp.float32) * 0.5

    def coarsen(values, first, halve):
        half = values.shape[0] // 2
        rows = values.shape[1]
        pair[0:half, 0:rows, :] = pair_planes(values)
        top = pair[0:half, pl.ds(first, 8, stride=2), :]
        top = top + pair[0:half, pl.ds(first + 1, 8, stride=2), :]
        return lanes_dot(top, halve)

    def pack(level, which, fields):
        r, bz, pitch = HALO[level], DEPTH[level], PITCH[level]
        joined = len(fields) == 1
        low = jnp.bitwise_and(lane, pitch - 1)
        for side in range(2):
            start = bz - r if side else 0
            acc = jnp.zeros((SIZE[level], LANES), jnp.float32)
            for x in range(SIZE[level]):
                for f, values in enumerate(fields):
                    place = f * pitch + x * r
                    shift = (place - start) % LANES
                    moved = values[x] if shift == 0 else pltpu.roll(values[x], shift, 1)
                    seat = low if joined else lane - f * pitch
                    acc = jnp.where((seat >= x * r) & (seat < x * r + r), moved, acc)
            zs[which][side, :, :] = acc

    def unpack(level, which, f):
        n, r, bz = SIZE[level], HALO[level], DEPTH[level] % LANES
        planes = []
        for p in range(PLANES[level]):
            block, x = divmod(p - r + n, n)
            seat = f * PITCH[level] + x * r
            down = (LANES - r - seat) % LANES
            up = (bz - seat) % LANES
            below, above = zr[which][0, block], zr[which][1, block]
            below = pltpu.roll(below, down, 1) if down else below
            above = pltpu.roll(above, up, 1) if up else above
            inner = jnp.where((lane >= bz) & (lane < bz + r), above, 0.0)
            planes.append(jnp.where(lane >= LANES - r, below, inner))
        return jnp.stack(planes, axis=0)

    def span(step, n, r):
        return ((0, n), (n - r, r), (0, r))[step]

    unsent = {}

    def drain(sem, rows):
        pltpu.make_async_copy(tally.at[pl.ds(0, rows)], tally.at[pl.ds(0, rows)], sem).wait()

    def sent(turn_set):
        if turn_set in unsent:
            drain(send_sem.at[turn_set], unsent.pop(turn_set))

    def exchange(level, which, blocks, turn_set):
        n, r, row = SIZE[level], HALO[level], ROW[level]
        sent(turn_set)
        sems = dict(send_sem=send_sem.at[turn_set], recv_sem=recv_sem.at[turn_set])
        copies, rows = [], 0
        for o in TALL:
            sy, cy = span(o[1], n, r)
            up = o[2] > 0
            rows += cy
            copies.append(
                pltpu.make_async_remote_copy(
                    src_ref=zs[which].at[1 if up else 0, pl.ds(sy, cy)],
                    dst_ref=zr[which].at[
                        0 if up else 1, 1 - o[0], pl.ds(row + sy - o[1] * n, cy)
                    ],
                    device_id=device(o),
                    device_id_type=MESH,
                    **sems,
                )
            )
        for o in FLAT:
            sx, cx = span(o[0], n, r)
            sy, cy = span(o[1], n, r)
            for block in blocks:
                rows += cx * cy
                copies.append(
                    pltpu.make_async_remote_copy(
                        src_ref=block.at[pl.ds(r + sx, cx), pl.ds(row + sy, cy)],
                        dst_ref=block.at[
                            pl.ds(r + sx - o[0] * n, cx), pl.ds(row + sy - o[1] * n, cy)
                        ],
                        device_id=device(o),
                        device_id_type=MESH,
                        **sems,
                    )
                )
        for copy in copies:
            copy.start()
        unsent[turn_set] = rows
        return turn_set, rows

    def finish(pending):
        drain(recv_sem.at[pending[0]], pending[1])

    def domain(level, r, row, rows):
        n, bz = SIZE[level], DEPTH[level]
        lanes = 256 if level == 0 else LANES
        px = iota((n + 2 * r, 1, 1), 0) - r
        py = iota((1, rows, 1), 1) - row
        pz = iota((1, 1, lanes), 2)
        pz = jnp.where(pz < bz + 32, pz, pz - lanes)
        ok = None
        for p, here, count, size in ((px, gx, NX, n), (py, gy, NY, n), (pz, gz, NZ, bz)):
            at = p + here * size
            good = (p >= -r) & (p < size + r) & (at >= 0) & (at < count * size)
            ok = good if ok is None else ok & good
        return ok

    def extended(level):
        return domain(level, HALO[level], ROW[level], ROWS[level])

    def presmooth(b, d, inside, extra, r):
        n = b.shape[0] - 2 * r
        diag = 6.0 + d
        w = jnp.where(inside, RELAX / diag, 0.0)
        v = sweep(w * b, b[1:-1], w[1:-1])
        near = v[r - extra - 2 : r + n + extra]
        mid = slice(r - extra, r + n + extra)
        rest = b[mid] - diag[mid] * near[1:-1] + neighbour_sum(near)
        return w, v, rest[:, :, :LANES]

    own_damping = []
    for load in loads:
        load.wait()
    d_own = ed[pl.ds(HALO[0], n), pl.ds(ROW[0], n), :]
    pack(0, 0, (eb[pl.ds(HALO[0], n), pl.ds(ROW[0], n), :], d_own))
    pl.semaphore_wait(barrier, len(peers))
    copies = exchange(0, 0, (eb, ed), 0)

    values = d_own
    for level in range(LEVELS - 1):
        coarse = coarsen(values, 0, whole)
        own_damping.append(coarse)
        values = coarse
    d_last = own_damping[-1]
    own_nodes = (iota((8, LANES), 0) < SIZE[3]) & (iota((8, LANES), 1) < DEPTH[3])
    last_scale = 0.25 ** (LEVELS - 1) / (SIZE[3] * SIZE[3] * DEPTH[3])

    def block_mean(planes, good):
        total = jnp.where(good, sum(planes[k] for k in range(planes.shape[0])), 0.0)
        total = jnp.sum(jnp.sum(total, axis=0, keepdims=True), axis=1, keepdims=True)
        return total * last_scale

    damping_mean = block_mean(d_last, own_nodes)

    finish(copies)
    b0 = jnp.concatenate([eb[...], unpack(0, 0, 0)], axis=2)
    d0 = jnp.concatenate([ed[...], unpack(0, 0, 1)], axis=2)
    bx[0][...] = b0
    wx[0][...], vx[0][...], remainder = presmooth(b0, d0, extended(0), 0, HALO[0])

    def joined_rows(level, fields):
        out = fields[0]
        for k, values in enumerate(fields[1:], 1):
            out = jnp.where(lane < k * PITCH[level], out, pltpu.roll(values, k * PITCH[level], 2))
        return out

    def send(level, which, block, values, turn_set):
        n, r, row = SIZE[level], HALO[level], ROW[level]
        block[pl.ds(r, n), pl.ds(row, n), :] = values
        pack(level, which, (values,))
        return exchange(level, which, (block,), turn_set)

    def received(level, which, block, count):
        e = block[...]
        fields = []
        for f in range(count):
            own = pltpu.roll(e, LANES - f * PITCH[level], 2) if f else e
            fields.append(jnp.where(lane < DEPTH[level], own, unpack(level, which, f)))
        return fields

    coarse = coarsen(remainder, ROW[0], whole)
    finish(send(1, 1, e1, joined_rows(1, (coarse, own_damping[0]))[:, : SIZE[1]], 1))
    b, d = received(1, 1, e1, 2)
    bx[1][...] = b
    wx[1][...], vx[1][...], remainder = presmooth(b, d, extended(1), 4, HALO[1])
    b = coarsen(remainder, ROW[1] - 4, turned)
    d = coarsen(d[HALO[1] - 4 : HALO[1] + SIZE[1] + 4], ROW[1] - 4, turned)
    _, v, remainder = presmooth(b, d, domain(2, 2, 2, 8), 0, 2)
    n = SIZE[2]
    own = joined_rows(2, (b[2 : 2 + n], d[2 : 2 + n], v[1 : 1 + n]))
    own = own[:, 2 : 2 + n]
    coarse = coarsen(remainder, 2, whole)

    d3 = coarsen(d, 0, turned)
    at_row, at_lane = iota((1, 8, LANES), 1), iota((1, 8, LANES), 2)
    near_lane = (at_lane <= DEPTH[3]) | (at_lane == LANES - 1)
    none = jnp.zeros((1, 8, LANES), jnp.float32)
    d3 = jnp.where((at_row >= 1) & (at_row <= 4) & near_lane, pltpu.roll(d3, 1, 1), 0.0)
    d3 = jnp.concatenate([none, d3, none], axis=0)
    mine = (at_row >= 2) & (at_row < 2 + SIZE[3]) & (at_lane < DEPTH[3])
    b3 = jnp.where(mine, pltpu.roll(coarse, 2, 1), 0.0)
    b3 = jnp.concatenate([none, none, b3, none, none], axis=0)
    diag = 6.0 + d3
    w3 = jnp.where(domain(3, 2, 2, 8), RELAX / diag, 0.0)
    v = sweep(w3 * b3, b3[1:-1], w3[1:-1])
    near = jnp.concatenate([none, none, v, none, none], axis=0)
    parts = pair_planes(b3 - diag * near[1:-1] + neighbour_sum(near))
    to = iota((LANES, LANES), 1)
    side = jnp.where(source_lane < DEPTH[3], 0, jnp.where(source_lane < 64, 1, -1))
    seat = (to % NZ == gz + side) & (to < 3 * NZ)
    seat = seat & ((source_lane < DEPTH[3] + 2) | (source_lane >= LANES - 2))
    parts = lanes_dot(parts, seat.astype(jnp.float32)) * last_scale
    parts = jnp.where((at_row < 6) & (at_row // 2 == at_lane // NZ), parts, 0.0)
    parts = jnp.sum(parts, axis=1, keepdims=True)

    def rows_of(values):
        row = iota((8, LANES), 0)
        out = jnp.where(row == 0, values[0], jnp.where(row == 1, values[1], values[2]))
        return jnp.where(row < 3, out, 0.0)

    def send_line(axis, src, dst):
        here, count = (gx, gy, gz)[axis], counts[axis]
        for k in range(1, count):
            offset = tuple(k if a == axis else 0 for a in range(3))
            pltpu.make_async_remote_copy(
                src_ref=src.at[pl.ds(0, 3)],
                dst_ref=dst.at[here, pl.ds(0, 3)],
                send_sem=line_send.at[axis],
                recv_sem=line_recv.at[axis],
                device_id=device(offset),
                device_id_type=MESH,
            ).start()

    def line_rows(axis, own, dst):
        drain(line_recv.at[axis], 3 * (counts[axis] - 1))
        here, count = (gx, gy, gz)[axis], counts[axis]
        places = iota(dst.shape, 0)
        got = jnp.where(places == here, own, dst[...])
        return jnp.where((places < count) & (iota(dst.shape, 1) < 3), got, 0.0)

    own0 = jnp.where(lane < 64, rows_of(parts), damping_mean)
    row0[...] = own0
    send_line(2, row0, g1)
    copies = send(3, 3, e3, joined_rows(3, (coarse, own_damping[2]))[:, : SIZE[3]], 2)
    hidden = send(2, 2, u2, own, 3)

    got = jnp.sum(line_rows(2, own0, g1), axis=0)
    at_y = lane // NZ + (gy - 1)
    moved = jnp.where((lane < 3 * NZ) & (at_y >= 0) & (at_y < NY), got, 0.0)
    moved = pltpu.roll(moved, lax.rem((gy - 1) * NZ + LANES, LANES), 1)
    own1 = jnp.where(lane < 64, moved, got)
    row1[...] = own1
    send_line(1, row1, g2)

    def relay(turn_set, moves):
        rows = 0
        for o, first, size, target in moves:
            rows += math.prod(size)
            pltpu.make_async_remote_copy(
                src_ref=u3.at[tuple(pl.ds(f, c) for f, c in zip(first, size))],
                dst_ref=u3.at[tuple(pl.ds(f, c) for f, c in zip(target, size))],
                send_sem=send_sem.at[turn_set],
                recv_sem=recv_sem.at[turn_set],
                device_id=device(o),
                device_id_type=MESH,
            ).start()
        unsent[turn_set] = rows
        return turn_set, rows

    finish(copies)
    b, d = received(3, 3, e3, 2)
    _, v, _ = presmooth(b, d, extended(3), 0, HALO[3])
    n, row = SIZE[3], ROW[3]
    block3 = jnp.where(lane < 32, b, jnp.where(lane < 64, pltpu.roll(d, 32, 2), 0.0))[2 : 2 + n]
    block3 = jnp.where(lane < 64, block3, pltpu.roll(v[1 : 1 + n], 64, 2))
    u3[1, pl.ds(4, n), pl.ds(4, n), :] = block3[:, row : row + n]
    steps = (-2, -1, 1, 2)
    copies = relay(4, [((0, 0, o), (1, 4, 4), (1, n, n), (1 - o, 4, 4)) for o in (-1, 1)])
    got = jnp.sum(line_rows(1, own1, g2), axis=0)
    own2 = got
    row2[...] = own2
    send_line(0, row2, g3)
    finish(copies)
    copies = relay(
        5, [((o, 0, 0), (0, 4, 4), (3, n, n), (0, 4 - n * o, 4)) for o in steps]
    )
    finish(hidden)
    b, d, smooth2 = received(2, 2, u2, 3)
    bx[2][...] = b
    wx[2][...] = jnp.where(extended(2), RELAX / (6.0 + d), 0.0)
    vx[2][...] = jnp.where(extended(2), smooth2, 0.0)
    finish(copies)
    copies = relay(
        6, [((0, o, 0), (0, 0, 4), (3, 8 + n, n), (0, 0, 4 - n * o)) for o in steps]
    )
    table_load.wait()
    dot = functools.partial(jnp.dot, precision=HI, preferred_element_type=jnp.float32)
    table_x = tab_ref[0:NXP, 0:NXP]
    table_yz = tab_ref[pl.ds(16, LANES), :]
    eigen = tab_ref[pl.ds(16 + LANES, NXP), :]
    from_row = iota((NXP, 8 * NXP), 1)
    sums = (from_row // 8 + from_row % 8 - 1 == iota((NXP, 8 * NXP), 0)) & (from_row % 8 < 3)
    table_sum = dot(table_x, sums.astype(jnp.float32))
    got = line_rows(0, own2, g3)
    mean = jnp.sum(got, axis=0)[0:1] * (1.0 / (NX * NY * NZ))
    mean = jnp.where(lane < 64, pltpu.roll(mean, 64, 1), 0.0)
    got = jnp.where(lane < NY * NZ, got.reshape(8 * NXP, LANES), 0.0)
    spectrum = dot(dot(table_sum, got), table_yz)
    spectrum = spectrum / (eigen + mean)
    coarse = dot(dot(table_x, spectrum), table_yz)

    pick = iota((16, NXP), 1) == gx - 2 + iota((16, NXP), 0) // 2
    along_x = dot(pick.astype(jnp.float32), coarse)
    wanted = iota((16, LANES), 1) // NZ == gy - 2 + iota((16, LANES), 0) // 2
    spread = jnp.stack(
        [
            jnp.where(wanted, jnp.broadcast_to(along_x[p : p + 1], (16, LANES)), 0.0)
            for p in range(8 + SIZE[3])
        ],
        axis=0,
    )
    seat = source_lane % NZ == gz + jnp.where(to < DEPTH[3], 0, jnp.where(to < 64, 1, -1))
    correction = lanes_dot(spread, seat.astype(jnp.float32))

    def postsmooth(level, v, start):
        for _ in range(2):
            start = start + 1
            count = v.shape[0] - 2
            v = sweep(v, bx[level][pl.ds(start, count)], wx[level][pl.ds(start, count)])
        return v

    finish(copies)
    fields = []
    for f in range(3):
        here, below, above = (u3[k] for k in (1, 0, 2))
        here = pltpu.roll(here, LANES - 32 * f, 2) if f == 1 or f == 2 else here
        below = pltpu.roll(below, LANES - DEPTH[3] - 32 * f, 2)
        above = pltpu.roll(above, (LANES + DEPTH[3] - 32 * f) % LANES, 2)
        outer = jnp.where(lane < DEPTH[3] + 4, above, jnp.where(lane >= LANES - 4, below, 0.0))
        fields.append(jnp.where(lane < DEPTH[3], here, outer))
    b3, d3, smooth3 = fields
    inside = domain(3, 4, 4, 16)
    w3 = jnp.where(inside, RELAX / (6.0 + d3), 0.0)
    v = jnp.where(inside, smooth3 + correction, 0.0)
    v = sweep(v, b3[1:-1], w3[1:-1])
    v = sweep(v, b3[2:-2], w3[2:-2])

    def refined(level, v, first):
        lanes = 256 if level == 0 else LANES
        table = refine_table(lanes, DEPTH[level] + 32)
        planes = v.shape[0]
        wide = lanes_dot(v, table)
        count = ROWS[level] // 2
        parts = []
        for half in range(lanes // LANES):
            piece = wide[:, first : first + count, half * LANES : (half + 1) * LANES]
            fine0[0:planes, pl.ds(0, count, stride=2), :] = piece
            fine0[0:planes, pl.ds(1, count, stride=2), :] = piece
            parts.append(fine0[0:planes, 0 : ROWS[level], :])
        full = parts[0] if len(parts) == 1 else jnp.concatenate(parts, axis=2)
        full = jnp.broadcast_to(full[:, None], (planes, 2, ROWS[level], lanes))
        return full.reshape(2 * planes, ROWS[level], lanes)

    v = vx[2][...] + refined(2, v, 4 - ROW[2] // 2)
    v = postsmooth(2, v, 0)
    correction = refined(1, v, ROW[2] - ROW[1] // 2)
    v = vx[1][pl.ds(2, 14)] + correction[1:-1]
    v = postsmooth(1, v, 3)
    correction = refined(0, v, ROW[1] - ROW[0] // 2)
    v = vx[0][...] + correction
    v = postsmooth(0, v, 1)
    for axis in range(3):
        drain(line_send.at[axis], 3 * (counts[axis] - 1))
    for turn_set in list(unsent):
        sent(turn_set)
    out_ref[...] = v[:, ROW[0] : ROW[0] + SIZE[0], :LANES]


def tables(counts):
    def sine(points):
        index = np.arange(1, points + 1)
        return math.sqrt(2.0 / (points + 1)) * np.sin(
            math.pi * index[:, None] * index[None, :] / (points + 1)
        )

    def eigen(points, spacing):
        index = np.arange(1, points + 1)
        return (2.0 - 2.0 * np.cos(math.pi * index / (points + 1))) / (spacing * spacing)

    nx, ny, nz = counts
    out = np.zeros((16 + LANES + 16, LANES))
    out[:nx, :nx] = sine(nx)
    out[16 : 16 + ny * nz, : ny * nz] = np.kron(sine(ny), sine(nz))
    plane = eigen(ny, 16.0)[:, None] + eigen(nz, 128.0)[None, :]
    out[16 + LANES :] = 1.0
    out[16 + LANES : 16 + LANES + nx, : ny * nz] = eigen(nx, 16.0)[:, None] + plane.reshape(1, -1)
    return out.astype(np.float32)


def solution(mesh):
    counts = tuple(mesh.shape[a] for a in ("gx", "gy", "gz"))
    NXP = max(8, counts[0])
    f32 = jnp.float32

    def local(divergence, damping):
        ext = [(p, r, LANES) for p, r in zip(PLANES, ROWS)]
        levels = (0, 1, 2, 3)
        wide = [(p, r, 256 if k == 0 else LANES) for k, (p, r) in enumerate(zip(PLANES, ROWS))][:3]
        inner = [(p - 2, r, z) for p, r, z in wide]
        inner[2] = wide[2]
        shapes = [ext[0], ext[0], ext[1], ext[3], ext[2], (3, 10, 16, LANES), (32 + LANES, LANES)]
        shapes += [(2, SIZE[k], LANES) for k in levels]
        shapes += [(2, 3, ROWS[k], LANES) for k in levels]
        shapes += wide + wide + inner
        shapes += [(8, 24, LANES), (12, 24, LANES)]
        shapes += [(8, LANES)] * 3
        shapes += [(8, 8, LANES), (8, 8, LANES), (NXP, 8, LANES), (1024, LANES)]
        dma = pltpu.SemaphoreType.DMA
        sems = [dma((7,)), dma((7,)), dma((3,)), dma((3,)), dma((3,))]
        return pl.pallas_call(
            functools.partial(kernel, counts),
            out_shape=jax.ShapeDtypeStruct(divergence.shape, f32),
            in_specs=[
                pl.BlockSpec(memory_space=pltpu.HBM),
                pl.BlockSpec(memory_space=pltpu.HBM),
                pl.BlockSpec(memory_space=pltpu.HBM),
            ],
            out_specs=pl.BlockSpec(memory_space=pltpu.VMEM),
            scratch_shapes=[pltpu.VMEM(s, f32) for s in shapes] + sems,
            compiler_params=pltpu.CompilerParams(
                collective_id=0, has_side_effects=True
            ),
            name="vcycle",
        )(divergence, damping, jnp.asarray(tables(counts)))

    spec = P("gx", "gy", "gz")
    return jax.shard_map(
        local, mesh=mesh, in_specs=(spec, spec), out_specs=spec, check_vma=False
    )
```

```python
import functools
import itertools
import math

import jax
import jax.numpy as jnp
import numpy as np
from jax import lax
from jax.experimental import pallas as pl
from jax.experimental.pallas import tpu as pltpu
from jax.sharding import PartitionSpec as P

MESH = pl.DeviceIdType.MESH
HI = lax.Precision.HIGHEST
LEVELS = 4
LANES = 128
RELAX = 2.0 / 3.0
SIZE = (16, 8, 4, 2)
DEPTH = (128, 64, 32, 16)
HALO = (3, 6, 4, 2)
ROW = (4, 8, 4, 2)
PLANES = tuple(n + 2 * r for n, r in zip(SIZE, HALO))
ROWS = (24, 24, 16, 8)
PITCH = (64, 64, 32, 64)
DEEP = (3, 6, 4, 5)
OFFSETS = [o for o in itertools.product((-1, 0, 1), repeat=3) if o != (0, 0, 0)]
FLAT = [o for o in OFFSETS if o[2] == 0]
TALL = [o for o in OFFSETS if o[2] != 0]
FAR = [
    (x, y, 0)
    for x in range(-2, 3)
    for y in range(-2, 3)
    if (x, y) != (0, 0) and abs(x) + abs(y) < 4
]


def iota(shape, axis):
    return lax.broadcasted_iota(jnp.int32, shape, axis)


def neighbour_sum(v):
    c = v[1:-1]
    rows, lanes = c.shape[1], c.shape[2]
    total = v[2:] + v[:-2]
    total = total + (pltpu.roll(c, 1, 1) + pltpu.roll(c, rows - 1, 1))
    return total + (pltpu.roll(c, 1, 2) + pltpu.roll(c, lanes - 1, 2))


def sweep(v, b, w):
    return v[1:-1] * (1.0 / 3.0) + w * (b + neighbour_sum(v))


def pair_planes(v):
    n = v.shape[0]
    halves = v.reshape(n // 2, 2, v.shape[1], v.shape[2])
    return halves[:, 0] + halves[:, 1]


def lanes_dot(v, table):
    planes, rows, lanes = v.shape
    out = jnp.dot(
        v.reshape(planes * rows, lanes), table, precision=HI, preferred_element_type=jnp.float32
    )
    return out.reshape(planes, rows, table.shape[1])


def refine_table(lanes, turn):
    fine = iota((LANES, lanes), 1)
    place = jnp.where(fine < turn, fine, fine - lanes)
    coarse = jnp.bitwise_and(place + 2 * LANES, 1)
    coarse = (place + 2 * LANES - coarse) // 2 % LANES
    return (iota((LANES, lanes), 0) == coarse).astype(jnp.float32)


def kernel(counts, b_hbm, d_hbm, tab_hbm, out_ref, *refs):
    NX, NY, NZ = counts
    NXP = max(8, NX)
    it = iter(refs)
    eb, ed, e1, e3, u2, u3, tab_ref = (next(it) for _ in range(7))
    zs = [next(it) for _ in range(4)]
    zr = [next(it) for _ in range(4)]
    bx = [next(it) for _ in range(3)]
    wx = [next(it) for _ in range(3)]
    vx = [next(it) for _ in range(3)]
    pair, fine0 = next(it), next(it)
    row0, row1, row2, g1, g2, g3 = (next(it) for _ in range(6))
    tally = next(it)
    send_sem, recv_sem, line_send, line_recv, in_sem = (next(it) for _ in range(5))

    gx, gy, gz = lax.axis_index("gx"), lax.axis_index("gy"), lax.axis_index("gz")

    places = {}
    for name, here, count in zip(("gx", "gy", "gz"), (gx, gy, gz), counts):
        places[name, 0] = here
        for step in range(1, count):
            moved = here + step
            places[name, step] = jnp.where(moved >= count, moved - count, moved)

    def device(offset):
        return tuple(
            places[name, step % count]
            for name, count, step in zip(("gx", "gy", "gz"), counts, offset)
        )

    for ref in (eb, ed, e1, e3, u2, u3, pair, *zs, *zr):
        ref[...] = jnp.zeros(ref.shape, jnp.float32)
    n = SIZE[0]
    loads = []
    for k, (src, dst) in enumerate(((b_hbm, eb), (d_hbm, ed))):
        load = pltpu.make_async_copy(
            src, dst.at[pl.ds(HALO[0], n), pl.ds(ROW[0], n)], in_sem.at[k]
        )
        load.start()
        loads.append(load)
    table_load = pltpu.make_async_copy(tab_hbm.at[pl.ds(0, 32 + LANES)], tab_ref, in_sem.at[2])
    table_load.start()

    peers = set()
    for o in OFFSETS + FAR:
        peers.add(tuple(s % c for s, c in zip(o, counts)))
    for axis in range(3):
        for k in range(1, counts[axis]):
            peers.add(tuple(k if a == axis else 0 for a in range(3)))
    peers.discard((0, 0, 0))
    barrier = pltpu.get_barrier_semaphore()
    for o in sorted(peers):
        pl.semaphore_signal(barrier, inc=1, device_id=device(o), device_id_type=MESH)

    lane = iota((1, LANES), 1)
    source_lane = iota((LANES, LANES), 0)
    whole = (source_lane // 2 == iota((LANES, LANES), 1)).astype(jnp.float32) * 0.5
    turned = source_lane // 2 + jnp.where(source_lane < 96, 0, 64)
    turned = (turned == iota((LANES, LANES), 1)).astype(jnp.float32) * 0.5

    def coarsen(values, first, halve):
        half = values.shape[0] // 2
        rows = values.shape[1]
        pair[0:half, 0:rows, :] = pair_planes(values)
        top = pair[0:half, pl.ds(first, 8, stride=2), :]
        top = top + pair[0:half, pl.ds(first + 1, 8, stride=2), :]
        return lanes_dot(top, halve)

    def pack(level, which, fields):
        r, bz, pitch = DEEP[level], DEPTH[level], PITCH[level]
        joined = len(fields) == 1
        low = jnp.bitwise_and(lane, pitch - 1)
        for side in range(2):
            start = bz - r if side else 0
            acc = jnp.zeros((SIZE[level], LANES), jnp.float32)
            for x in range(SIZE[level]):
                for f, values in enumerate(fields):
                    place = f * pitch + x * r
                    shift = (place - start) % LANES
                    moved = values[x] if shift == 0 else pltpu.roll(values[x], shift, 1)
                    seat = low if joined else lane - f * pitch
                    acc = jnp.where((seat >= x * r) & (seat < x * r + r), moved, acc)
            zs[which][side, :, :] = acc

    def unpack(level, which, f):
        n, wide, bz, r = SIZE[level], HALO[level], DEPTH[level] % LANES, DEEP[level]
        planes = []
        for p in range(PLANES[level]):
            block, x = divmod(p - wide + n, n)
            seat = f * PITCH[level] + x * r
            down = (LANES - r - seat) % LANES
            up = (bz - seat) % LANES
            below, above = zr[which][0, block], zr[which][1, block]
            below = pltpu.roll(below, down, 1) if down else below
            above = pltpu.roll(above, up, 1) if up else above
            inner = jnp.where((lane >= bz) & (lane < bz + r), above, 0.0)
            planes.append(jnp.where(lane >= LANES - r, below, inner))
        return jnp.stack(planes, axis=0)

    def span(step, n, r):
        return ((0, n), (n - r, r), (0, r))[step]

    unsent = {}

    def drain(sem, rows):
        pltpu.make_async_copy(tally.at[pl.ds(0, rows)], tally.at[pl.ds(0, rows)], sem).wait()

    def sent(turn_set):
        if turn_set in unsent:
            drain(send_sem.at[turn_set], unsent.pop(turn_set))

    def exchange(level, which, blocks, turn_set):
        n, r, row = SIZE[level], HALO[level], ROW[level]
        sent(turn_set)
        sems = dict(send_sem=send_sem.at[turn_set], recv_sem=recv_sem.at[turn_set])
        copies, rows = [], 0
        for o in TALL:
            sy, cy = span(o[1], n, r)
            up = o[2] > 0
            rows += cy
            copies.append(
                pltpu.make_async_remote_copy(
                    src_ref=zs[which].at[1 if up else 0, pl.ds(sy, cy)],
                    dst_ref=zr[which].at[
                        0 if up else 1, 1 - o[0], pl.ds(row + sy - o[1] * n, cy)
                    ],
                    device_id=device(o),
                    device_id_type=MESH,
                    **sems,
                )
            )
        for o in FLAT:
            sx, cx = span(o[0], n, r)
            sy, cy = span(o[1], n, r)
            for block in blocks:
                rows += cx * cy
                copies.append(
                    pltpu.make_async_remote_copy(
                        src_ref=block.at[pl.ds(r + sx, cx), pl.ds(row + sy, cy)],
                        dst_ref=block.at[
                            pl.ds(r + sx - o[0] * n, cx), pl.ds(row + sy - o[1] * n, cy)
                        ],
                        device_id=device(o),
                        device_id_type=MESH,
                        **sems,
                    )
                )
        for copy in copies:
            copy.start()
        unsent[turn_set] = rows
        return turn_set, rows

    def finish(pending):
        drain(recv_sem.at[pending[0]], pending[1])

    def domain(level, r, row, rows, deep):
        n, bz = SIZE[level], DEPTH[level]
        lanes = 256 if level == 0 else LANES
        px = iota((n + 2 * r, 1, 1), 0) - r
        py = iota((1, rows, 1), 1) - row
        pz = iota((1, 1, lanes), 2)
        pz = jnp.where(pz < bz + 32, pz, pz - lanes)
        ok = None
        for p, here, count, size, halo in (
            (px, gx, NX, n, r),
            (py, gy, NY, n, r),
            (pz, gz, NZ, bz, deep),
        ):
            at = p + here * size
            good = (p >= -halo) & (p < size + halo) & (at >= 0) & (at < count * size)
            ok = good if ok is None else ok & good
        return ok

    def extended(level):
        return domain(level, HALO[level], ROW[level], ROWS[level], DEEP[level])

    def presmooth(b, d, inside, extra, r):
        n = b.shape[0] - 2 * r
        diag = 6.0 + d
        w = jnp.where(inside, RELAX / diag, 0.0)
        v = sweep(w * b, b[1:-1], w[1:-1])
        near = v[r - extra - 2 : r + n + extra]
        mid = slice(r - extra, r + n + extra)
        rest = b[mid] - diag[mid] * near[1:-1] + neighbour_sum(near)
        return w, v, rest[:, :, :LANES]

    own_damping = []
    for load in loads:
        load.wait()
    d_own = ed[pl.ds(HALO[0], n), pl.ds(ROW[0], n), :]
    pack(0, 0, (eb[pl.ds(HALO[0], n), pl.ds(ROW[0], n), :], d_own))
    pl.semaphore_wait(barrier, len(peers))
    copies = exchange(0, 0, (eb, ed), 0)

    values = d_own
    for level in range(LEVELS - 1):
        coarse = coarsen(values, 0, whole)
        own_damping.append(coarse)
        values = coarse
    d_last = own_damping[-1]
    own_nodes = (iota((8, LANES), 0) < SIZE[3]) & (iota((8, LANES), 1) < DEPTH[3])
    last_scale = 0.25 ** (LEVELS - 1) / (SIZE[3] * SIZE[3] * DEPTH[3])

    def block_mean(planes, good):
        total = jnp.where(good, sum(planes[k] for k in range(planes.shape[0])), 0.0)
        total = jnp.sum(jnp.sum(total, axis=0, keepdims=True), axis=1, keepdims=True)
        return total * last_scale

    damping_mean = block_mean(d_last, own_nodes)

    finish(copies)
    b0 = jnp.concatenate([eb[...], unpack(0, 0, 0)], axis=2)
    d0 = jnp.concatenate([ed[...], unpack(0, 0, 1)], axis=2)
    bx[0][...] = b0
    wx[0][...], vx[0][...], remainder = presmooth(b0, d0, extended(0), 0, HALO[0])

    def joined_rows(level, fields):
        out = fields[0]
        for k, values in enumerate(fields[1:], 1):
            out = jnp.where(lane < k * PITCH[level], out, pltpu.roll(values, k * PITCH[level], 2))
        return out

    def send(level, which, block, values, turn_set):
        n, r, row = SIZE[level], HALO[level], ROW[level]
        block[pl.ds(r, n), pl.ds(row, n), :] = values
        pack(level, which, (values,))
        return exchange(level, which, (block,), turn_set)

    def received(level, which, block, count):
        e = block[...]
        fields = []
        for f in range(count):
            own = pltpu.roll(e, LANES - f * PITCH[level], 2) if f else e
            fields.append(jnp.where(lane < DEPTH[level], own, unpack(level, which, f)))
        return fields

    coarse = coarsen(remainder, ROW[0], whole)
    finish(send(1, 1, e1, joined_rows(1, (coarse, own_damping[0]))[:, : SIZE[1]], 1))
    b, d = received(1, 1, e1, 2)
    bx[1][...] = b
    wx[1][...], vx[1][...], remainder = presmooth(b, d, extended(1), 4, HALO[1])
    b = coarsen(remainder, ROW[1] - 4, turned)
    d = coarsen(d[HALO[1] - 4 : HALO[1] + SIZE[1] + 4], ROW[1] - 4, turned)
    _, v, remainder = presmooth(b, d, domain(2, 2, 2, 8, 2), 0, 2)
    n = SIZE[2]
    own = joined_rows(2, (b[2 : 2 + n], d[2 : 2 + n], v[1 : 1 + n]))
    own = own[:, 2 : 2 + n]
    coarse = coarsen(remainder, 2, whole)

    d3 = coarsen(d, 0, turned)
    at_row, at_lane = iota((1, 8, LANES), 1), iota((1, 8, LANES), 2)
    near_lane = (at_lane <= DEPTH[3]) | (at_lane == LANES - 1)
    none = jnp.zeros((1, 8, LANES), jnp.float32)
    d3 = jnp.where((at_row >= 1) & (at_row <= 4) & near_lane, pltpu.roll(d3, 1, 1), 0.0)
    d3 = jnp.concatenate([none, d3, none], axis=0)
    mine = (at_row >= 2) & (at_row < 2 + SIZE[3]) & (at_lane < DEPTH[3])
    b3 = jnp.where(mine, pltpu.roll(coarse, 2, 1), 0.0)
    b3 = jnp.concatenate([none, none, b3, none, none], axis=0)
    diag = 6.0 + d3
    w3 = jnp.where(domain(3, 2, 2, 8, 2), RELAX / diag, 0.0)
    v = sweep(w3 * b3, b3[1:-1], w3[1:-1])
    near = jnp.concatenate([none, none, v, none, none], axis=0)
    parts = pair_planes(b3 - diag * near[1:-1] + neighbour_sum(near))
    to = iota((LANES, LANES), 1)
    side = jnp.where(source_lane < DEPTH[3], 0, jnp.where(source_lane < 64, 1, -1))
    seat = (to % NZ == gz + side) & (to < 3 * NZ)
    seat = seat & ((source_lane < DEPTH[3] + 2) | (source_lane >= LANES - 2))
    parts = lanes_dot(parts, seat.astype(jnp.float32)) * last_scale
    parts = jnp.where((at_row < 6) & (at_row // 2 == at_lane // NZ), parts, 0.0)
    parts = jnp.sum(parts, axis=1, keepdims=True)

    def rows_of(values):
        row = iota((8, LANES), 0)
        out = jnp.where(row == 0, values[0], jnp.where(row == 1, values[1], values[2]))
        return jnp.where(row < 3, out, 0.0)

    def send_line(axis, src, dst):
        here, count = (gx, gy, gz)[axis], counts[axis]
        for k in range(1, count):
            offset = tuple(k if a == axis else 0 for a in range(3))
            pltpu.make_async_remote_copy(
                src_ref=src.at[pl.ds(0, 3)],
                dst_ref=dst.at[here, pl.ds(0, 3)],
                send_sem=line_send.at[axis],
                recv_sem=line_recv.at[axis],
                device_id=device(offset),
                device_id_type=MESH,
            ).start()

    def line_rows(axis, own, dst):
        drain(line_recv.at[axis], 3 * (counts[axis] - 1))
        here, count = (gx, gy, gz)[axis], counts[axis]
        places = iota(dst.shape, 0)
        got = jnp.where(places == here, own, dst[...])
        return jnp.where((places < count) & (iota(dst.shape, 1) < 3), got, 0.0)

    own0 = jnp.where(lane < 64, rows_of(parts), damping_mean)
    row0[...] = own0
    send_line(2, row0, g1)
    copies = send(3, 3, e3, joined_rows(3, (coarse, own_damping[2]))[:, : SIZE[3]], 2)
    hidden = send(2, 2, u2, own, 3)

    got = jnp.sum(line_rows(2, own0, g1), axis=0)
    at_y = lane // NZ + (gy - 1)
    moved = jnp.where((lane < 3 * NZ) & (at_y >= 0) & (at_y < NY), got, 0.0)
    moved = pltpu.roll(moved, lax.rem((gy - 1) * NZ + LANES, LANES), 1)
    own1 = jnp.where(lane < 64, moved, got)
    row1[...] = own1
    send_line(1, row1, g2)

    finish(copies)
    b, d = received(3, 3, e3, 2)
    _, v, _ = presmooth(b, d, extended(3), 0, HALO[3])
    n, row = SIZE[3], ROW[3]
    block3 = None
    for f, values in enumerate((b[2 : 2 + n], d[2 : 2 + n], v[1 : 1 + n])):
        values = jnp.where(lane < 24, values, pltpu.roll(values, 32, 2))
        if f:
            block3 = jnp.where(lane < 32 * f, block3, pltpu.roll(values, 32 * f, 2))
        else:
            block3 = values
    u3[pl.ds(4, n), pl.ds(4, n), :] = block3[:, row : row + n]
    for o in FAR:
        pltpu.make_async_remote_copy(
            src_ref=u3.at[pl.ds(4, n), pl.ds(4, n)],
            dst_ref=u3.at[pl.ds(4 - n * o[0], n), pl.ds(4 - n * o[1], n)],
            send_sem=send_sem.at[4],
            recv_sem=recv_sem.at[4],
            device_id=device(o),
            device_id_type=MESH,
        ).start()
    unsent[4] = len(FAR) * n * n
    copies = (4, len(FAR) * n * n)

    own2 = jnp.sum(line_rows(1, own1, g2), axis=0)
    row2[...] = own2
    send_line(0, row2, g3)
    finish(hidden)
    b, d, smooth2 = received(2, 2, u2, 3)
    bx[2][...] = b
    wx[2][...] = jnp.where(extended(2), RELAX / (6.0 + d), 0.0)
    vx[2][...] = jnp.where(extended(2), smooth2, 0.0)
    table_load.wait()
    dot = functools.partial(jnp.dot, precision=HI, preferred_element_type=jnp.float32)
    table_x = tab_ref[0:NXP, 0:NXP]
    table_yz = tab_ref[pl.ds(16, LANES), :]
    eigen = tab_ref[pl.ds(16 + LANES, NXP), :]
    from_row = iota((NXP, 8 * NXP), 1)
    sums = (from_row // 8 + from_row % 8 - 1 == iota((NXP, 8 * NXP), 0)) & (from_row % 8 < 3)
    table_sum = dot(table_x, sums.astype(jnp.float32))
    pick = iota((16, NXP), 1) == gx - 2 + iota((16, NXP), 0) // 2
    table_pick = dot(pick.astype(jnp.float32), table_x)
    finish(copies)
    e = u3[...]
    fields = []
    for f in range(3):
        values = pltpu.roll(e, LANES - 32 * f, 2) if f else e
        outer = jnp.where(lane >= LANES - 4, pltpu.roll(values, 96, 2), 0.0)
        fields.append(jnp.where(lane < DEPTH[3] + 4, values, outer))
    b3, d3, smooth3 = fields
    inside = domain(3, 4, 4, 16, 4)
    w3 = jnp.where(inside, RELAX / (6.0 + d3), 0.0)

    got = line_rows(0, own2, g3)
    mean = jnp.sum(got, axis=0)[0:1] * (1.0 / (NX * NY * NZ))
    mean = jnp.where(lane < 64, pltpu.roll(mean, 64, 1), 0.0)
    got = jnp.where(lane < NY * NZ, got.reshape(8 * NXP, LANES), 0.0)
    spectrum = dot(dot(table_sum, got), table_yz)
    spectrum = spectrum / (eigen + mean)
    along_x = dot(dot(table_pick, spectrum), table_yz)

    wanted = iota((16, LANES), 1) // NZ == gy - 2 + iota((16, LANES), 0) // 2
    spread = jnp.stack(
        [
            jnp.where(wanted, jnp.broadcast_to(along_x[p : p + 1], (16, LANES)), 0.0)
            for p in range(8 + SIZE[3])
        ],
        axis=0,
    )
    seat = source_lane % NZ == gz + jnp.where(to < DEPTH[3], 0, jnp.where(to < 64, 1, -1))
    correction = lanes_dot(spread, seat.astype(jnp.float32))

    def postsmooth(level, v, start):
        for _ in range(2):
            start = start + 1
            count = v.shape[0] - 2
            v = sweep(v, bx[level][pl.ds(start, count)], wx[level][pl.ds(start, count)])
        return v

    v = jnp.where(inside, smooth3 + correction, 0.0)
    v = sweep(v, b3[1:-1], w3[1:-1])
    v = sweep(v, b3[2:-2], w3[2:-2])

    def refined(level, v, first):
        lanes = 256 if level == 0 else LANES
        table = refine_table(lanes, DEPTH[level] + 32)
        planes = v.shape[0]
        wide = lanes_dot(v, table)
        count = ROWS[level] // 2
        parts = []
        for half in range(lanes // LANES):
            piece = wide[:, first : first + count, half * LANES : (half + 1) * LANES]
            fine0[0:planes, pl.ds(0, count, stride=2), :] = piece
            fine0[0:planes, pl.ds(1, count, stride=2), :] = piece
            parts.append(fine0[0:planes, 0 : ROWS[level], :])
        full = parts[0] if len(parts) == 1 else jnp.concatenate(parts, axis=2)
        full = jnp.broadcast_to(full[:, None], (planes, 2, ROWS[level], lanes))
        return full.reshape(2 * planes, ROWS[level], lanes)

    v = vx[2][...] + refined(2, v, 4 - ROW[2] // 2)
    v = postsmooth(2, v, 0)
    correction = refined(1, v, ROW[2] - ROW[1] // 2)
    v = vx[1][pl.ds(2, 14)] + correction[1:-1]
    v = postsmooth(1, v, 3)
    correction = refined(0, v, ROW[1] - ROW[0] // 2)
    v = vx[0][...] + correction
    v = postsmooth(0, v, 1)
    for axis in range(3):
        drain(line_send.at[axis], 3 * (counts[axis] - 1))
    for turn_set in list(unsent):
        sent(turn_set)
    out_ref[...] = v[:, ROW[0] : ROW[0] + SIZE[0], :LANES]


def tables(counts):
    def sine(points):
        index = np.arange(1, points + 1)
        return math.sqrt(2.0 / (points + 1)) * np.sin(
            math.pi * index[:, None] * index[None, :] / (points + 1)
        )

    def eigen(points, spacing):
        index = np.arange(1, points + 1)
        return (2.0 - 2.0 * np.cos(math.pi * index / (points + 1))) / (spacing * spacing)

    nx, ny, nz = counts
    out = np.zeros((1024, LANES))
    out[:nx, :nx] = sine(nx)
    out[16 : 16 + ny * nz, : ny * nz] = np.kron(sine(ny), sine(nz))
    plane = eigen(ny, 16.0)[:, None] + eigen(nz, 128.0)[None, :]
    out[16 + LANES : 32 + LANES] = 1.0
    out[16 + LANES : 16 + LANES + nx, : ny * nz] = eigen(nx, 16.0)[:, None] + plane.reshape(1, -1)
    return out.astype(np.float32)


def solution(mesh):
    counts = tuple(mesh.shape[a] for a in ("gx", "gy", "gz"))
    NXP = max(8, counts[0])
    f32 = jnp.float32

    def local(divergence, damping):
        ext = [(p, r, LANES) for p, r in zip(PLANES, ROWS)]
        levels = (0, 1, 2, 3)
        wide = [(p, r, 256 if k == 0 else LANES) for k, (p, r) in enumerate(zip(PLANES, ROWS))][:3]
        inner = [(p - 2, r, z) for p, r, z in wide]
        inner[2] = wide[2]
        shapes = [ext[0], ext[0], ext[1], ext[3], ext[2], (10, 16, LANES), (32 + LANES, LANES)]
        shapes += [(2, SIZE[k], LANES) for k in levels]
        shapes += [(2, 3, ROWS[k], LANES) for k in levels]
        shapes += wide + wide + inner
        shapes += [(8, 24, LANES), (12, 24, LANES)]
        shapes += [(8, LANES)] * 3
        shapes += [(8, 8, LANES), (8, 8, LANES), (NXP, 8, LANES), (1024, LANES)]
        dma = pltpu.SemaphoreType.DMA
        sems = [dma((5,)), dma((5,)), dma((3,)), dma((3,)), dma((3,))]
        return pl.pallas_call(
            functools.partial(kernel, counts),
            out_shape=jax.ShapeDtypeStruct(divergence.shape, f32),
            in_specs=[
                pl.BlockSpec(memory_space=pltpu.HBM),
                pl.BlockSpec(memory_space=pltpu.HBM),
                pl.BlockSpec(memory_space=pltpu.HBM),
            ],
            out_specs=pl.BlockSpec(memory_space=pltpu.VMEM),
            scratch_shapes=[pltpu.VMEM(s, f32) for s in shapes] + sems,
            compiler_params=pltpu.CompilerParams(
                collective_id=0, has_side_effects=True, vmem_limit_bytes=55000 * 1024
            ),
            name="vcycle",
        )(divergence, damping, jnp.asarray(tables(counts)))

    spec = P("gx", "gy", "gz")
    return jax.shard_map(
        local, mesh=mesh, in_specs=(spec, spec), out_specs=spec, check_vma=False
    )
```

```python
import functools
import itertools
import math

import jax
import jax.numpy as jnp
import numpy as np
from jax import lax
from jax.experimental import pallas as pl
from jax.experimental.pallas import tpu as pltpu
from jax.sharding import PartitionSpec as P

MESH = pl.DeviceIdType.MESH
HI = lax.Precision.HIGHEST
LEVELS = 4
LANES = 128
RELAX = 2.0 / 3.0
SIZE = (16, 8, 4, 2)
DEPTH = (128, 64, 32, 16)
HALO = (3, 6, 4, 2)
ROW = (4, 8, 4, 2)
PLANES = tuple(n + 2 * r for n, r in zip(SIZE, HALO))
ROWS = (24, 24, 16, 8)
PITCH = (64, 64, 32, 64)
DEEP = (3, 6, 4, 5)
OFFSETS = [o for o in itertools.product((-1, 0, 1), repeat=3) if o != (0, 0, 0)]
FLAT = [o for o in OFFSETS if o[2] == 0]
TALL = [o for o in OFFSETS if o[2] != 0]
FAR = [
    (x, y, 0)
    for x in range(-2, 3)
    for y in range(-2, 3)
    if (x, y) != (0, 0) and abs(x) + abs(y) < 4
]


def iota(shape, axis):
    return lax.broadcasted_iota(jnp.int32, shape, axis)


def neighbour_sum(v):
    c = v[1:-1]
    rows, lanes = c.shape[1], c.shape[2]
    total = v[2:] + v[:-2]
    total = total + (pltpu.roll(c, 1, 1) + pltpu.roll(c, rows - 1, 1))
    return total + (pltpu.roll(c, 1, 2) + pltpu.roll(c, lanes - 1, 2))


def sweep(v, b, w):
    return v[1:-1] * (1.0 / 3.0) + w * (b + neighbour_sum(v))


def pair_planes(v):
    n = v.shape[0]
    halves = v.reshape(n // 2, 2, v.shape[1], v.shape[2])
    return halves[:, 0] + halves[:, 1]


def lanes_dot(v, table):
    planes, rows, lanes = v.shape
    flat = v.reshape(planes * rows, lanes)
    parts = []
    for _ in range(3):
        parts.append(flat.astype(jnp.bfloat16))
        flat = flat - parts[-1].astype(jnp.float32)
    table = table.astype(jnp.bfloat16)
    dot = functools.partial(jnp.dot, preferred_element_type=jnp.float32)
    out = dot(parts[0], table) + (dot(parts[1], table) + dot(parts[2], table))
    return out.reshape(planes, rows, table.shape[1])


def refine_table(lanes, turn):
    fine = iota((LANES, lanes), 1)
    place = jnp.where(fine < turn, fine, fine - lanes)
    coarse = jnp.bitwise_and(place + 2 * LANES, 1)
    coarse = (place + 2 * LANES - coarse) // 2 % LANES
    return (iota((LANES, lanes), 0) == coarse).astype(jnp.float32)


def kernel(counts, b_hbm, d_hbm, tab_hbm, out_ref, *refs):
    NX, NY, NZ = counts
    NXP = max(8, NX)
    it = iter(refs)
    e0, e1, e3, u2, u3, tab_ref = (next(it) for _ in range(6))
    zs = [next(it) for _ in range(4)]
    zr = [next(it) for _ in range(4)]
    bx = [next(it) for _ in range(3)]
    wx = [next(it) for _ in range(3)]
    vx = [next(it) for _ in range(3)]
    pair, fine0 = next(it), next(it)
    row1, row2, g1, g3 = (next(it) for _ in range(4))
    tally = next(it)
    send_sem, recv_sem, line_send, line_recv, in_sem = (next(it) for _ in range(5))

    gx, gy, gz = lax.axis_index("gx"), lax.axis_index("gy"), lax.axis_index("gz")

    places = {}
    for name, here, count in zip(("gx", "gy", "gz"), (gx, gy, gz), counts):
        places[name, 0] = here
        for step in range(1, count):
            moved = here + step
            places[name, step] = jnp.where(moved >= count, moved - count, moved)

    def device(offset):
        return tuple(
            places[name, step % count]
            for name, count, step in zip(("gx", "gy", "gz"), counts, offset)
        )

    for ref in (e0, e1, e3, u2, u3, pair, *zs, *zr):
        ref[...] = jnp.zeros(ref.shape, jnp.float32)
    n = SIZE[0]
    loads = []
    for k, src in enumerate((b_hbm, d_hbm)):
        load = pltpu.make_async_copy(
            src, e0.at[k, pl.ds(HALO[0], n), pl.ds(ROW[0], n)], in_sem.at[k]
        )
        load.start()
        loads.append(load)
    table_load = pltpu.make_async_copy(tab_hbm.at[pl.ds(0, 32 + LANES)], tab_ref, in_sem.at[2])
    table_load.start()

    peers = set()
    for o in OFFSETS + FAR:
        peers.add(tuple(s % c for s, c in zip(o, counts)))
    line = [(k, 0, 0) for k in range(NX)]
    plane = [(0, j, k) for j in range(NY) for k in range(NZ)]
    peers.update(line, plane)
    peers.discard((0, 0, 0))
    barrier = pltpu.get_barrier_semaphore()
    def steps(o):
        return sum(min(s, c - s) for s, c in zip(o, counts))

    for o in sorted(peers, key=lambda o: (steps(o), o)):
        pl.semaphore_signal(barrier, inc=1, device_id=device(o), device_id_type=MESH)

    lane = iota((1, LANES), 1)
    source_lane = iota((LANES, LANES), 0)
    whole = (source_lane // 2 == iota((LANES, LANES), 1)).astype(jnp.float32) * 0.5
    turned = source_lane // 2 + jnp.where(source_lane < 96, 0, 64)
    turned = (turned == iota((LANES, LANES), 1)).astype(jnp.float32) * 0.5

    def coarsen(values, first, halve):
        half = values.shape[0] // 2
        rows = values.shape[1]
        pair[0:half, 0:rows, :] = pair_planes(values)
        top = pair[0:half, pl.ds(first, 8, stride=2), :]
        top = top + pair[0:half, pl.ds(first + 1, 8, stride=2), :]
        return lanes_dot(top, halve)

    def pack(level, which, fields):
        r, bz, pitch = DEEP[level], DEPTH[level], PITCH[level]
        joined = len(fields) == 1
        low = jnp.bitwise_and(lane, pitch - 1)
        for side in range(2):
            start = bz - r if side else 0
            acc = jnp.zeros((SIZE[level], LANES), jnp.float32)
            for x in range(SIZE[level]):
                for f, values in enumerate(fields):
                    place = f * pitch + x * r
                    shift = (place - start) % LANES
                    moved = values[x] if shift == 0 else pltpu.roll(values[x], shift, 1)
                    seat = low if joined else lane - f * pitch
                    acc = jnp.where((seat >= x * r) & (seat < x * r + r), moved, acc)
            zs[which][side, :, :] = acc

    def unpack(level, which, f):
        n, wide, bz, r = SIZE[level], HALO[level], DEPTH[level] % LANES, DEEP[level]
        planes = []
        for p in range(PLANES[level]):
            block, x = divmod(p - wide + n, n)
            seat = f * PITCH[level] + x * r
            down = (LANES - r - seat) % LANES
            up = (bz - seat) % LANES
            below, above = zr[which][0, block], zr[which][1, block]
            below = pltpu.roll(below, down, 1) if down else below
            above = pltpu.roll(above, up, 1) if up else above
            inner = jnp.where((lane >= bz) & (lane < bz + r), above, 0.0)
            planes.append(jnp.where(lane >= LANES - r, below, inner))
        return jnp.stack(planes, axis=0)

    def span(step, n, r):
        return ((0, n), (n - r, r), (0, r))[step]

    unsent = {}

    def drain(sem, rows):
        pltpu.make_async_copy(tally.at[pl.ds(0, rows)], tally.at[pl.ds(0, rows)], sem).wait()

    def sent(turn_set):
        if turn_set in unsent:
            drain(send_sem.at[turn_set], unsent.pop(turn_set))

    def exchange(level, which, block, turn_set):
        n, r, row = SIZE[level], HALO[level], ROW[level]
        sent(turn_set)
        sems = dict(send_sem=send_sem.at[turn_set], recv_sem=recv_sem.at[turn_set])
        copies, rows = [], 0
        for o in TALL:
            sy, cy = span(o[1], n, r)
            up = o[2] > 0
            rows += cy
            copies.append(
                pltpu.make_async_remote_copy(
                    src_ref=zs[which].at[1 if up else 0, pl.ds(sy, cy)],
                    dst_ref=zr[which].at[
                        0 if up else 1, 1 - o[0], pl.ds(row + sy - o[1] * n, cy)
                    ],
                    device_id=device(o),
                    device_id_type=MESH,
                    **sems,
                )
            )
        for o in FLAT:
            sx, cx = span(o[0], n, r)
            sy, cy = span(o[1], n, r)
            fields = (pl.ds(0, 2),) if level == 0 else ()
            rows += cx * cy * (1 + len(fields))
            copies.append(
                pltpu.make_async_remote_copy(
                    src_ref=block.at[fields + (pl.ds(r + sx, cx), pl.ds(row + sy, cy))],
                    dst_ref=block.at[
                        fields + (pl.ds(r + sx - o[0] * n, cx), pl.ds(row + sy - o[1] * n, cy))
                    ],
                    device_id=device(o),
                    device_id_type=MESH,
                    **sems,
                )
            )
        for copy in copies:
            copy.start()
        unsent[turn_set] = rows
        return turn_set, rows

    def finish(pending):
        drain(recv_sem.at[pending[0]], pending[1])

    def domain(level, r, row, rows, deep):
        n, bz = SIZE[level], DEPTH[level]
        lanes = 256 if level == 0 else LANES
        px = iota((n + 2 * r, 1, 1), 0) - r
        py = iota((1, rows, 1), 1) - row
        pz = iota((1, 1, lanes), 2)
        pz = jnp.where(pz < bz + 32, pz, pz - lanes)
        ok = None
        for p, here, count, size, halo in (
            (px, gx, NX, n, r),
            (py, gy, NY, n, r),
            (pz, gz, NZ, bz, deep),
        ):
            at = p + here * size
            good = (p >= -halo) & (p < size + halo) & (at >= 0) & (at < count * size)
            ok = good if ok is None else ok & good
        return ok

    def extended(level):
        return domain(level, HALO[level], ROW[level], ROWS[level], DEEP[level])

    def presmooth(b, d, inside, extra, r):
        n = b.shape[0] - 2 * r
        diag = 6.0 + d
        w = jnp.where(inside, RELAX / diag, 0.0)
        v = sweep(w * b, b[1:-1], w[1:-1])
        near = v[r - extra - 2 : r + n + extra]
        mid = slice(r - extra, r + n + extra)
        rest = b[mid] - diag[mid] * near[1:-1] + neighbour_sum(near)
        return w, v, rest[:, :, :LANES]

    own_damping = []
    for load in loads:
        load.wait()
    d_own = e0[1, pl.ds(HALO[0], n), pl.ds(ROW[0], n), :]
    pack(0, 0, (e0[0, pl.ds(HALO[0], n), pl.ds(ROW[0], n), :], d_own))
    pl.semaphore_wait(barrier, len(peers))
    copies = exchange(0, 0, e0, 0)

    values = d_own
    for level in range(LEVELS - 1):
        coarse = coarsen(values, 0, whole)
        own_damping.append(coarse)
        values = coarse
    d_last = own_damping[-1]
    own_nodes = (iota((8, LANES), 0) < SIZE[3]) & (iota((8, LANES), 1) < DEPTH[3])
    last_scale = 0.25 ** (LEVELS - 1) / (SIZE[3] * SIZE[3] * DEPTH[3])

    def block_mean(planes, good):
        total = jnp.where(good, sum(planes[k] for k in range(planes.shape[0])), 0.0)
        total = jnp.sum(jnp.sum(total, axis=0, keepdims=True), axis=1, keepdims=True)
        return total * last_scale

    damping_mean = block_mean(d_last, own_nodes)

    finish(copies)
    b0 = jnp.concatenate([e0[0], unpack(0, 0, 0)], axis=2)
    d0 = jnp.concatenate([e0[1], unpack(0, 0, 1)], axis=2)
    bx[0][...] = b0
    wx[0][...], vx[0][...], remainder = presmooth(b0, d0, extended(0), 0, HALO[0])

    def joined_rows(level, fields):
        out = fields[0]
        for k, values in enumerate(fields[1:], 1):
            out = jnp.where(lane < k * PITCH[level], out, pltpu.roll(values, k * PITCH[level], 2))
        return out

    def send(level, which, block, values, turn_set):
        n, r, row = SIZE[level], HALO[level], ROW[level]
        block[pl.ds(r, n), pl.ds(row, n), :] = values
        pack(level, which, (values,))
        return exchange(level, which, block, turn_set)

    def received(level, which, block, count):
        e = block[...]
        fields = []
        for f in range(count):
            own = pltpu.roll(e, LANES - f * PITCH[level], 2) if f else e
            fields.append(jnp.where(lane < DEPTH[level], own, unpack(level, which, f)))
        return fields

    coarse = coarsen(remainder, ROW[0], whole)
    finish(send(1, 1, e1, joined_rows(1, (coarse, own_damping[0]))[:, : SIZE[1]], 1))
    b, d = received(1, 1, e1, 2)
    bx[1][...] = b
    wx[1][...], vx[1][...], remainder = presmooth(b, d, extended(1), 4, HALO[1])
    b = coarsen(remainder, ROW[1] - 4, turned)
    d = coarsen(d[HALO[1] - 4 : HALO[1] + SIZE[1] + 4], ROW[1] - 4, turned)
    _, v, remainder = presmooth(b, d, domain(2, 2, 2, 8, 2), 0, 2)
    n = SIZE[2]
    own = joined_rows(2, (b[2 : 2 + n], d[2 : 2 + n], v[1 : 1 + n]))
    own = own[:, 2 : 2 + n]
    coarse = coarsen(remainder, 2, whole)

    d3 = coarsen(d, 0, turned)
    at_row, at_lane = iota((1, 8, LANES), 1), iota((1, 8, LANES), 2)
    near_lane = (at_lane <= DEPTH[3]) | (at_lane == LANES - 1)
    none = jnp.zeros((1, 8, LANES), jnp.float32)
    d3 = jnp.where((at_row >= 1) & (at_row <= 4) & near_lane, pltpu.roll(d3, 1, 1), 0.0)
    d3 = jnp.concatenate([none, d3, none], axis=0)
    mine = (at_row >= 2) & (at_row < 2 + SIZE[3]) & (at_lane < DEPTH[3])
    b3 = jnp.where(mine, pltpu.roll(coarse, 2, 1), 0.0)
    b3 = jnp.concatenate([none, none, b3, none, none], axis=0)
    diag = 6.0 + d3
    w3 = jnp.where(domain(3, 2, 2, 8, 2), RELAX / diag, 0.0)
    v = sweep(w3 * b3, b3[1:-1], w3[1:-1])
    near = jnp.concatenate([none, none, v, none, none], axis=0)
    parts = pair_planes(b3 - diag * near[1:-1] + neighbour_sum(near))
    to = iota((LANES, LANES), 1)
    side = jnp.where(source_lane < DEPTH[3], 0, jnp.where(source_lane < 64, 1, -1))
    seat = (to % NZ == gz + side) & (to < 3 * NZ)
    seat = seat & ((source_lane < DEPTH[3] + 2) | (source_lane >= LANES - 2))
    parts = lanes_dot(parts, seat.astype(jnp.float32)) * last_scale
    parts = jnp.where((at_row < 6) & (at_row // 2 == at_lane // NZ), parts, 0.0)
    parts = jnp.sum(parts, axis=1, keepdims=True)

    def rows_of(values):
        row = iota((8, LANES), 0)
        out = jnp.where(row == 0, values[0], jnp.where(row == 1, values[1], values[2]))
        return jnp.where(row < 3, out, 0.0)

    def send_sums(stage, src, dst, here, offsets):
        offsets = [o for o in offsets if o != (0, 0, 0)]
        for o in sorted(offsets, key=steps, reverse=True):
            pltpu.make_async_remote_copy(
                src_ref=src.at[pl.ds(0, 3)],
                dst_ref=dst.at[here, pl.ds(0, 3)],
                send_sem=line_send.at[stage],
                recv_sem=line_recv.at[stage],
                device_id=device(o),
                device_id_type=MESH,
            ).start()

    def sums(stage, own, dst, here, count):
        drain(line_recv.at[stage], 3 * (count - 1))
        places = iota(dst.shape, 0)
        got = jnp.where(places == here, own, dst[...])
        return jnp.where((places < count) & (iota(dst.shape, 1) < 3), got, 0.0)

    moved = rows_of(parts)
    at_y = lane // NZ + (gy - 1)
    moved = jnp.where((lane < 3 * NZ) & (at_y >= 0) & (at_y < NY), moved, 0.0)
    moved = pltpu.roll(moved, lax.rem((gy - 1) * NZ + LANES, LANES), 1)
    own1 = jnp.where(lane < 64, moved, damping_mean)
    row1[...] = own1
    here1 = gy * NZ + gz
    send_sums(0, row1, g1, here1, plane)
    copies = send(3, 3, e3, joined_rows(3, (coarse, own_damping[2]))[:, : SIZE[3]], 2)
    hidden = send(2, 2, u2, own, 3)

    finish(copies)
    b, d = received(3, 3, e3, 2)
    _, v, _ = presmooth(b, d, extended(3), 0, HALO[3])
    n, row = SIZE[3], ROW[3]
    block3 = None
    for f, values in enumerate((b[2 : 2 + n], d[2 : 2 + n], v[1 : 1 + n])):
        values = jnp.where(lane < 24, values, pltpu.roll(values, 32, 2))
        if f:
            block3 = jnp.where(lane < 32 * f, block3, pltpu.roll(values, 32 * f, 2))
        else:
            block3 = values
    u3[pl.ds(4, n), pl.ds(4, n), :] = block3[:, row : row + n]
    for o in FAR:
        pltpu.make_async_remote_copy(
            src_ref=u3.at[pl.ds(4, n), pl.ds(4, n)],
            dst_ref=u3.at[pl.ds(4 - n * o[0], n), pl.ds(4 - n * o[1], n)],
            send_sem=send_sem.at[4],
            recv_sem=recv_sem.at[4],
            device_id=device(o),
            device_id_type=MESH,
        ).start()
    unsent[4] = len(FAR) * n * n
    copies = (4, len(FAR) * n * n)

    own2 = jnp.sum(sums(0, own1, g1, here1, NY * NZ), axis=0)
    row2[...] = own2
    send_sums(1, row2, g3, gx, line)
    finish(hidden)
    b, d, smooth2 = received(2, 2, u2, 3)
    bx[2][...] = b
    wx[2][...] = jnp.where(extended(2), RELAX / (6.0 + d), 0.0)
    vx[2][...] = jnp.where(extended(2), smooth2, 0.0)
    table_load.wait()
    dot = functools.partial(jnp.dot, precision=HI, preferred_element_type=jnp.float32)
    table_x = tab_ref[0:NXP, 0:NXP]
    table_yz = tab_ref[pl.ds(16, LANES), :]
    eigen = tab_ref[pl.ds(16 + LANES, NXP), :]
    from_row = iota((NXP, 8 * NXP), 1)
    picks = (from_row // 8 + from_row % 8 - 1 == iota((NXP, 8 * NXP), 0)) & (from_row % 8 < 3)
    table_sum = dot(table_x, picks.astype(jnp.float32))
    pick = iota((16, NXP), 1) == gx - 2 + iota((16, NXP), 0) // 2
    table_pick = dot(pick.astype(jnp.float32), table_x)
    finish(copies)
    e = u3[...]
    fields = []
    for f in range(3):
        values = pltpu.roll(e, LANES - 32 * f, 2) if f else e
        outer = jnp.where(lane >= LANES - 4, pltpu.roll(values, 96, 2), 0.0)
        fields.append(jnp.where(lane < DEPTH[3] + 4, values, outer))
    b3, d3, smooth3 = fields
    inside = domain(3, 4, 4, 16, 4)
    w3 = jnp.where(inside, RELAX / (6.0 + d3), 0.0)

    got = sums(1, own2, g3, gx, NX)
    mean = jnp.sum(got, axis=0)[0:1] * (1.0 / (NX * NY * NZ))
    mean = jnp.where(lane < 64, pltpu.roll(mean, 64, 1), 0.0)
    got = jnp.where(lane < NY * NZ, got.reshape(8 * NXP, LANES), 0.0)
    spectrum = dot(dot(table_sum, got), table_yz)
    spectrum = spectrum / (eigen + mean)
    along_x = dot(dot(table_pick, spectrum), table_yz)

    wanted = iota((16, LANES), 1) // NZ == gy - 2 + iota((16, LANES), 0) // 2
    spread = jnp.stack(
        [
            jnp.where(wanted, jnp.broadcast_to(along_x[p : p + 1], (16, LANES)), 0.0)
            for p in range(8 + SIZE[3])
        ],
        axis=0,
    )
    seat = source_lane % NZ == gz + jnp.where(to < DEPTH[3], 0, jnp.where(to < 64, 1, -1))
    correction = lanes_dot(spread, seat.astype(jnp.float32))

    def postsmooth(level, v, start):
        for _ in range(2):
            start = start + 1
            count = v.shape[0] - 2
            v = sweep(v, bx[level][pl.ds(start, count)], wx[level][pl.ds(start, count)])
        return v

    v = jnp.where(inside, smooth3 + correction, 0.0)
    v = sweep(v, b3[1:-1], w3[1:-1])
    v = sweep(v, b3[2:-2], w3[2:-2])

    def refined(level, v, first):
        lanes = 256 if level == 0 else LANES
        table = refine_table(lanes, DEPTH[level] + 32)
        planes = v.shape[0]
        wide = lanes_dot(v, table)
        count = ROWS[level] // 2
        parts = []
        for half in range(lanes // LANES):
            piece = wide[:, first : first + count, half * LANES : (half + 1) * LANES]
            fine0[0:planes, pl.ds(0, count, stride=2), :] = piece
            fine0[0:planes, pl.ds(1, count, stride=2), :] = piece
            parts.append(fine0[0:planes, 0 : ROWS[level], :])
        full = parts[0] if len(parts) == 1 else jnp.concatenate(parts, axis=2)
        full = jnp.broadcast_to(full[:, None], (planes, 2, ROWS[level], lanes))
        return full.reshape(2 * planes, ROWS[level], lanes)

    v = vx[2][...] + refined(2, v, 4 - ROW[2] // 2)
    v = postsmooth(2, v, 0)
    correction = refined(1, v, ROW[2] - ROW[1] // 2)
    v = vx[1][pl.ds(2, 14)] + correction[1:-1]
    v = postsmooth(1, v, 3)
    correction = refined(0, v, ROW[1] - ROW[0] // 2)
    v = vx[0][...] + correction
    v = postsmooth(0, v, 1)
    drain(line_send.at[0], 3 * (NY * NZ - 1))
    drain(line_send.at[1], 3 * (NX - 1))
    for turn_set in list(unsent):
        sent(turn_set)
    out_ref[...] = v[:, ROW[0] : ROW[0] + SIZE[0], :LANES]


def tables(counts):
    def sine(points):
        index = np.arange(1, points + 1)
        return math.sqrt(2.0 / (points + 1)) * np.sin(
            math.pi * index[:, None] * index[None, :] / (points + 1)
        )

    def eigen(points, spacing):
        index = np.arange(1, points + 1)
        return (2.0 - 2.0 * np.cos(math.pi * index / (points + 1))) / (spacing * spacing)

    nx, ny, nz = counts
    out = np.zeros((1024, LANES))
    out[:nx, :nx] = sine(nx)
    out[16 : 16 + ny * nz, : ny * nz] = np.kron(sine(ny), sine(nz))
    plane = eigen(ny, 16.0)[:, None] + eigen(nz, 128.0)[None, :]
    out[16 + LANES : 32 + LANES] = 1.0
    out[16 + LANES : 16 + LANES + nx, : ny * nz] = eigen(nx, 16.0)[:, None] + plane.reshape(1, -1)
    return out.astype(np.float32)


def solution(mesh):
    counts = tuple(mesh.shape[a] for a in ("gx", "gy", "gz"))
    NXP = max(8, counts[0])
    f32 = jnp.float32

    def local(divergence, damping):
        ext = [(p, r, LANES) for p, r in zip(PLANES, ROWS)]
        levels = (0, 1, 2, 3)
        wide = [(p, r, 256 if k == 0 else LANES) for k, (p, r) in enumerate(zip(PLANES, ROWS))][:3]
        inner = [(p - 2, r, z) for p, r, z in wide]
        inner[2] = wide[2]
        shapes = [(2, *ext[0]), ext[1], ext[3], ext[2], (10, 16, LANES), (32 + LANES, LANES)]
        shapes += [(2, SIZE[k], LANES) for k in levels]
        shapes += [(2, 3, ROWS[k], LANES) for k in levels]
        shapes += wide + wide + inner
        shapes += [(8, 24, LANES), (12, 24, LANES)]
        shapes += [(8, LANES)] * 2
        shapes += [(64, 8, LANES), (NXP, 8, LANES), (1024, LANES)]
        dma = pltpu.SemaphoreType.DMA
        sems = [dma((5,)), dma((5,)), dma((2,)), dma((2,)), dma((3,))]
        return pl.pallas_call(
            functools.partial(kernel, counts),
            out_shape=jax.ShapeDtypeStruct(divergence.shape, f32),
            in_specs=[
                pl.BlockSpec(memory_space=pltpu.HBM),
                pl.BlockSpec(memory_space=pltpu.HBM),
                pl.BlockSpec(memory_space=pltpu.HBM),
            ],
            out_specs=pl.BlockSpec(memory_space=pltpu.VMEM),
            scratch_shapes=[pltpu.VMEM(s, f32) for s in shapes] + sems,
            compiler_params=pltpu.CompilerParams(
                collective_id=0, has_side_effects=True, vmem_limit_bytes=55000 * 1024
            ),
            name="vcycle",
        )(divergence, damping, jnp.asarray(tables(counts)))

    spec = P("gx", "gy", "gz")
    return jax.shard_map(
        local, mesh=mesh, in_specs=(spec, spec), out_specs=spec, check_vma=False
    )
```
